32 devices in a mesh: gx: 4 (over y, x), gy: 2 (over core), gz: 4 (over z).
Axes of the slice: x: 2, y: 2, z: 4, core: 2. Of those that a mesh axis runs over, the one named last changes fastest.
Arguments:
- old_pos: float32 [3, 4, 2, 4, 1536], P(None, 'gx', 'gy', 'gz'), may hold values from -6 to 6
- displacement: float32 [3, 4, 2, 4, 1536], P(None, 'gx', 'gy', 'gz'), may hold values from -0.3 to 0.3
- inv_mass: float32 [4, 2, 4, 1536], P('gx', 'gy', 'gz'), may hold values from 0.0625 to 1
- bond_head: int32 [4, 2, 4, 1024], P('gx', 'gy', 'gz'), may hold values from 0 to 1535, as said below
- bond_tail: int32 [4, 2, 4, 1024], P('gx', 'gy', 'gz'), may hold values from 0 to 1967, as said below
- send_list: int32 [4, 2, 4, 16], P('gx', 'gy', 'gz'), may hold values from 0 to 1535, as said below
Outputs:
- new_pos: float32 [3, 4, 2, 4, 1536], P(None, 'gx', 'gy', 'gz')
- multipliers: float32 [4, 2, 4, 1024], P('gx', 'gy', 'gz')
The draws below stay inside these ranges and needn't reach their ends.
Inputs may be any that keep to these rules, and one draw needn't show every extreme that they name: `bond_head`: distinct atoms of the owning domain; no atom is the first atom of two constraints. `bond_tail`: below 1536: an atom of the owning domain other than the constraint's first atom, never in send_list; otherwise a slot 1536 + block * 16 + entry with block in 0..26 other than 13, distinct within a domain; 192 constraints of each domain use such slots. `send_list`: distinct atoms of the domain; a send atom is never a constraint's first atom and never a local second atom.
All inputs are finite; a program needn't handle non-finite values.
Results may differ from the reference program's by a relative error of at most 0.0011.
Values sent between devices are 32-bit elements; how exact they have to be, the bound alone decides.
A program may use at most 64 MiB of HBM per device.

```python
import math
import jax
import jax.numpy as jnp
from jax import lax

ATOM_DEV = 1536
CON_DEV = 1024
SEND = 16
HALO_CON = 192
ORDER = 4
DOM_X = 4
DOM_Y = 2
DOM_Z = 4


def layout(key):
    base = jax.random.fold_in(key, 7)
    keys = jax.random.split(base, DOM_X * DOM_Y * DOM_Z)

    def domain(dom_key):
        key_perm, key_pick, key_slot = jax.random.split(dom_key, 3)
        order = jax.random.permutation(key_perm, ATOM_DEV).astype(jnp.int32)
        sending = order[ATOM_DEV - SEND:]
        heads = order[:CON_DEV]
        local_tail = order[1:CON_DEV + 1]
        picked = jax.random.permutation(key_pick, CON_DEV).astype(jnp.int32)[:HALO_CON]
        slots = jax.random.permutation(key_slot, 26 * SEND).astype(jnp.int32)[:HALO_CON]
        block = slots // SEND
        block = block + (block >= 13).astype(jnp.int32)
        halo_tail = ATOM_DEV + block * SEND + slots % SEND
        tails = local_tail.at[picked].set(halo_tail.astype(jnp.int32))
        return (sending, heads, tails)
    sending, heads, tails = jax.vmap(domain)(keys)
    return (sending.reshape(DOM_X, DOM_Y, DOM_Z, SEND).astype(jnp.int32), heads.reshape(DOM_X, DOM_Y, DOM_Z, CON_DEV).astype(jnp.int32), tails.reshape(DOM_X, DOM_Y, DOM_Z, CON_DEV).astype(jnp.int32))


def draw_bond_head(key, part):
    return layout(key)[1]


def draw_bond_tail(key, part):
    return layout(key)[2]


def draw_send_list(key, part):
    return layout(key)[0]


def block_scale(own_key, shape, cuts, smallest, high):
    def one(position, shards_of):
        heights = jax.random.uniform(jax.random.fold_in(jax.random.fold_in(own_key, 6), position), (shards_of,), jnp.float32, smallest / len(cuts), high / len(cuts))
        return jnp.repeat(jnp.exp(heights), shape[position] // shards_of).reshape((-1,) + (1,) * (len(shape) - position - 1))

    factor_of = one(*cuts[0])
    for cut in cuts[1:]:
        factor_of = factor_of * one(*cut)
    return factor_of


def scatter_about(rng, extent, width, most, pieces=(), kind=jnp.bfloat16):
    array = jax.random.normal(rng, extent, jnp.float32) * width
    if len(pieces) > 0:
        array = block_scale(rng, extent, pieces, -0.22, 0.18) * array
    return jnp.clip(array, min=-most, max=most).astype(kind)


def setup_inputs(seed: int = 0) -> dict:
    splits = jax.random.split(jax.random.key(seed), 7)
    old_pos = scatter_about(splits[0], (3, DOM_X, DOM_Y, DOM_Z, ATOM_DEV), 1.0, 6.0, ((1, 4), (2, 2), (3, 4)), jnp.float32)
    displacement = scatter_about(splits[1], (3, DOM_X, DOM_Y, DOM_Z, ATOM_DEV), 0.05, 0.3, ((1, 4), (2, 2), (3, 4)), jnp.float32)
    inv_mass = jnp.clip(jnp.exp(math.log(1.0) - 2.7725887 * jax.random.uniform(splits[2], (DOM_X, DOM_Y, DOM_Z, ATOM_DEV), jnp.float32) ** block_scale(splits[2], (DOM_X, DOM_Y, DOM_Z, ATOM_DEV), ((0, 4), (1, 2), (2, 4)), -0.2, 0.2)), 0.0625, 1.0)
    bond_head = draw_bond_head(jax.random.fold_in(splits[6], 71), 0)
    bond_tail = draw_bond_tail(jax.random.fold_in(splits[6], 71), 0)
    send_list = draw_send_list(jax.random.fold_in(splits[6], 71), 0)
    return {"old_pos": old_pos, "displacement": displacement, "inv_mass": inv_mass, "bond_head": bond_head, "bond_tail": bond_tail, "send_list": send_list}


def global_index(bond_head, bond_tail, send_list):
    axis_x = jnp.arange(DOM_X, dtype=jnp.int32)[:, None, None, None]
    axis_y = jnp.arange(DOM_Y, dtype=jnp.int32)[None, :, None, None]
    axis_z = jnp.arange(DOM_Z, dtype=jnp.int32)[None, None, :, None]
    flat_dev = (axis_x * DOM_Y + axis_y) * DOM_Z + axis_z
    head = (flat_dev * ATOM_DEV + bond_head).reshape(-1)
    is_local = bond_tail < ATOM_DEV
    slot = jnp.maximum(bond_tail - ATOM_DEV, 0)
    block = slot // SEND
    entry = slot % SEND
    near_x = (axis_x + block // 9 - 1) % DOM_X
    near_y = (axis_y + block // 3 % 3 - 1) % DOM_Y
    near_z = (axis_z + block % 3 - 1) % DOM_Z
    neigh = (near_x * DOM_Y + near_y) * DOM_Z + near_z
    remote = send_list.reshape(-1)[(neigh * SEND + entry).reshape(-1)].reshape(neigh.shape)
    tail = jnp.where(is_local, flat_dev * ATOM_DEV + bond_tail, neigh * ATOM_DEV + remote)
    return (head.astype(jnp.int32), tail.reshape(-1).astype(jnp.int32))

def reference(old_pos, displacement, inv_mass, bond_head, bond_tail, send_list):
    head, tail = global_index(bond_head, bond_tail, send_list)
    old_flat = old_pos.reshape(3, -1)
    pos_now = old_flat + displacement.reshape(3, -1)
    masses = inv_mass.reshape(1, -1)
    total_atoms = old_flat.shape[1]
    bond_old = old_flat[:, head] - old_flat[:, tail]
    length = jnp.maximum(jnp.sqrt(lax.optimization_barrier(jnp.sum(bond_old * bond_old, axis=0))), 0.5)
    direction = bond_old / length
    bond_scale = 1.0 / jnp.sqrt(masses[0, head] + masses[0, tail])

    def spread(values):
        weighted = bond_scale * values * direction
        buffer = jnp.zeros((3, total_atoms), jnp.float32)
        buffer = buffer.at[:, head].add(weighted).at[:, tail].add(-weighted)
        return masses * buffer

    def couple(values):
        shift_vec = spread(values)
        return values - bond_scale * lax.optimization_barrier(jnp.sum(direction * (shift_vec[:, head] - shift_vec[:, tail]), axis=0))

    def expand(right_side):
        solution = right_side
        series = right_side
        for sweep in range(ORDER):
            series = couple(series)
            solution = solution + series
        return solution
    right_one = bond_scale * (lax.optimization_barrier(jnp.sum(direction * (pos_now[:, head] - pos_now[:, tail]), axis=0)) - length)
    sol_one = expand(right_one)
    pos_now = pos_now - spread(sol_one)
    stretch = pos_now[:, head] - pos_now[:, tail]
    current = lax.optimization_barrier(jnp.sum(stretch * stretch, axis=0))
    target = jnp.sqrt(jnp.maximum(2.0 * length * length - current, 0.5 * length * length))
    sol_two = expand(bond_scale * (length - target))
    pos_now = pos_now - spread(sol_two)
    return (pos_now.reshape(old_pos.shape), (sol_one + sol_two).reshape(bond_head.shape))
```

```python
import functools

import jax
import jax.numpy as jnp
from jax import lax
from jax.experimental import pallas as pl
from jax.experimental.pallas import tpu as pltpu
from jax.sharding import PartitionSpec as P

ORDER = 4
LANES = 128
SUBS = 8
F32, BF16, I32 = jnp.float32, jnp.bfloat16, jnp.int32
MESH = pl.DeviceIdType.MESH
SYM = ((0, 0), (0, 1), (0, 2), (1, 1), (1, 2), (2, 2))


def dot_nt(left, right):
    return lax.dot_general(left, right, (((1,), (1,)), ((), ())), preferred_element_type=F32)


def dot_nn(left, right):
    return lax.dot_general(left, right, (((1,), (0,)), ((), ())), preferred_element_type=F32)


def wide(row, count=SUBS):
    return jnp.broadcast_to(row, (count, row.shape[1]))


def lanes_at(rows, index):
    return jnp.take_along_axis(rows, index, axis=1, mode="promise_in_bounds")


def subs_at(rows, index):
    return jnp.take_along_axis(rows, index, axis=0, mode="promise_in_bounds")


def split(value):
    high = value.astype(BF16).astype(F32)
    return high, value - high


def flips(n):
    return n >= 4 and n % 2 == 0


def routes(sizes):
    classes = [(a, b, c) for a in range(3) for b in range(3) for c in range(3)]
    direct, forth, back = [], [], []
    for cls in classes:
        direct.append(tuple((1 - c) for c in cls))
        forth.append(tuple((0, 1, -2)[c] if flips(n) else c - 1 for c, n in zip(cls, sizes)))
        back.append(tuple((0, 1, 2)[c] if flips(n) else 1 - c for c, n in zip(cls, sizes)))
    return classes, direct, forth, back


def kernel(
    axes, sizes, send_count,
    old_ref, move_ref, mass_ref, head_ref, tail_ref, send_ref,
    pos_ref, mult_ref,
    table, hot_head, hot_tail, hot_root, mask_tail, mask_root, stage,
    out0, in0, out1, in1, out2, in2, out3, in3, out4, in4,
    send_sem, recv_sem,
):
    atoms, bonds = old_ref.shape[-1], head_ref.shape[-1]
    atom_rows, bond_rows = atoms // LANES, bonds // LANES
    slot_rows = bond_rows + -(-(atoms - bonds) // LANES)
    width = send_count
    bits = width.bit_length() - 1
    classes, direct, forth, back = routes(sizes)
    centre = classes.index((1, 1, 1))
    hub_row = classes.index(tuple(0 if flips(n) else 1 for n in sizes))
    tiles = -(-len(classes) // SUBS)
    here = [lax.axis_index(name) for name in axes]
    turn = [1 - 2 * lax.rem(i, 2) if flips(n) else 1 for i, n in zip(here, sizes)]

    def nowhere(offset):
        return all(o % n == 0 for o, n in zip(offset, sizes))

    def target(offset):
        return tuple(
            lax.rem(i + o * s + 2 * n, n) for i, o, s, n in zip(here, offset, turn, sizes)
        )

    greet = []
    for group in (direct, forth, back):
        for offset in group:
            key = tuple(o % n for o, n in zip(offset, sizes))
            if any(key) and key not in [k for k, _ in greet]:
                greet.append((key, offset))
    barrier = pltpu.get_barrier_semaphore()
    for _, offset in greet:
        pl.semaphore_signal(barrier, inc=1, device_id=target(offset), device_id_type=MESH)

    sub = lax.broadcasted_iota(I32, (SUBS, LANES), 0)
    lane = lax.broadcasted_iota(I32, (SUBS, LANES), 1)
    group = lax.shift_right_logical(lane, bits)
    entry = lane & (width - 1)
    swap = (group - sub) & (SUBS - 1)
    unskew = (lane + width * sub) & (LANES - 1)

    def transpose8(x):
        x = pltpu.roll(x, 0, 1, stride=width, stride_axis=0)
        return lanes_at(subs_at(x, swap), unskew)

    def pick_rows(choice):
        index = jnp.zeros((SUBS, LANES), I32)
        for j, c in enumerate(choice):
            if c:
                index = jnp.where(sub == j, c, index)
        return index

    old = [old_ref[k, 0, 0].reshape(atom_rows, LANES) for k in range(3)]
    pos0 = [old[k] + move_ref[k, 0, 0].reshape(atom_rows, LANES) for k in range(3)]
    mass = mass_ref[0, 0].reshape(atom_rows, LANES)
    values = old + pos0 + [mass, jnp.zeros((atom_rows, LANES), F32)]
    for g, value in enumerate(values):
        for q in range(atom_rows):
            table[SUBS * q + g : SUBS * q + g + 1, :] = value[q : q + 1]
    send_row = jnp.concatenate(
        [send_ref[0, 0], jnp.zeros((1, LANES - send_count), I32)], axis=1
    )
    send_rep = lanes_at(wide(send_row), entry)
    send_tile, send_lane = lax.shift_right_logical(send_rep, 7), send_rep & (LANES - 1)
    found = jnp.zeros((SUBS, LANES), F32)
    for q in range(atom_rows):
        found = jnp.where(
            send_tile == q, lanes_at(table[SUBS * q : SUBS * q + SUBS, :], send_lane), found
        )
    found = jnp.sum(jnp.where(group == sub, found, 0.0), axis=0, keepdims=True)
    out0[0] = wide(found)
    for land in (in1, in3):
        for part in range(land.shape[0]):
            land[part, centre : centre + 1, :] = jnp.zeros((1, LANES), F32)
            land[part, len(classes) :, :] = jnp.zeros((SUBS * tiles - len(classes), LANES), F32)

    pl.semaphore_wait(barrier, len(greet))

    order = sorted(range(len(classes)), key=lambda r: -(classes[r][0] + classes[r][2]))

    def copies(step, source, landing, offsets, each, whole):
        started = []
        for row in order:
            if row == centre and not whole:
                continue
            line = row if each else 0
            if nowhere(offsets[row]):
                landing[:, row : row + 1, :] = source[:, line : line + 1, :]
                continue
            copy = pltpu.make_async_remote_copy(
                source.at[:, line], landing.at[:, row],
                send_sem.at[step, row], recv_sem.at[step, row],
                device_id=target(offsets[row]), device_id_type=MESH,
            )
            copy.start()
            started.append(copy)
        return started

    pending = []

    def arrive(started):
        for copy in started:
            copy.wait_recv()
        pending.extend(started)

    first = copies(0, out0, in0, direct, False, False)

    head = head_ref[0, 0].reshape(bond_rows, LANES)
    tail = tail_ref[0, 0].reshape(bond_rows, LANES)
    head_tile, head_lane = lax.shift_right_logical(head, 7), head & (LANES - 1)
    tail_tile, tail_lane = lax.shift_right_logical(tail, 7), tail & (LANES - 1)
    is_far = tail >= atoms
    slot = jnp.maximum(tail - atoms, 0)
    block = lax.shift_right_logical(slot, bits)
    one = lambda test: jnp.where(test, 1, 0)
    bx = one(block >= 9) + one(block >= 18)
    rest = block - 9 * bx
    by = one(rest >= 3) + one(rest >= 6)
    bz = rest - 3 * by
    place = [
        1 - s * (b - 1) if flips(n) else b
        for b, s, n in zip((bx, by, bz), turn, sizes)
    ]
    slot = ((place[0] * 3 + place[1]) * 3 + place[2]) * width + (slot & (width - 1))

    def gather(rows, tile, index, start=0.0, count=None):
        shape = index.shape
        total = jnp.full(shape, start, rows.dtype)
        for q in range(count or rows.shape[0]):
            total = jnp.where(tile == q, lanes_at(wide(rows[q : q + 1], shape[0]), index), total)
        return total

    deep = lax.broadcasted_iota(I32, (LANES, LANES), 0)
    across = lax.broadcasted_iota(I32, (LANES, LANES), 1)
    row16 = lax.broadcasted_iota(I32, (2 * SUBS, LANES), 0)
    parts = []
    for s in range(bond_rows):
        hot_head[:, s * LANES : (s + 1) * LANES] = jnp.where(
            deep == wide(head_lane[s : s + 1], LANES), 1.0, 0.0
        ).astype(BF16)
        number = lane[0:1] + (s * LANES + 1)
        high = (number - (number & 7)).astype(F32)
        low = (number & 7).astype(F32)
        match = row16 == wide(head_tile[s : s + 1], 2 * SUBS)
        parts.append(jnp.concatenate(
            [jnp.where(match, wide(high, 16), 0.0), jnp.where(match, wide(low, 16), 0.0)], axis=0
        ).astype(BF16))
    owner_of = dot_nt(jnp.concatenate(parts, axis=1), hot_head[...])
    owner_of = owner_of[:16] + owner_of[16:]
    free = jnp.where(owner_of == 0.0, 1.0, 0.0).astype(BF16)
    before = dot_nn(free, jnp.where(deep < across, 1.0, 0.0).astype(BF16))
    totals = dot_nn(free, jnp.ones((LANES, LANES), BF16))
    for q in range(atom_rows - 1):
        before = before + jnp.where(row16 > q, wide(totals[q : q + 1], 16), 0.0)
    place_of = jnp.where(owner_of > 0.0, owner_of - 1.0, before + float(bonds)).astype(I32)
    spot = gather(place_of, tail_tile, tail_lane, 0, atom_rows)
    spot = jnp.where(is_far, -1, spot)
    spot_tile, spot_lane = lax.shift_right_arithmetic(spot, 7), spot & (LANES - 1)

    label = jnp.where(is_far, slot, -1)
    for _ in range(ORDER + 1):
        label = jnp.where(is_far, slot, gather(label, spot_tile, spot_lane, -1))
    label_tile, label_lane = lax.shift_right_arithmetic(label, 7), label & (LANES - 1)

    def columns(index, dest):
        col = index.astype(F32).T
        line = lane[0:1].astype(F32)
        for s in range(bond_rows):
            dest[s * LANES : (s + 1) * LANES, :] = jnp.where(
                col[:, s : s + 1] == line, 1.0, 0.0
            ).astype(BF16)

    columns(spot_lane, hot_tail)
    columns(label_lane, hot_root)
    for s in range(bond_rows):
        mask_tail[16 * s : 16 * s + 16, :] = jnp.where(
            row16 == wide(spot_tile[s : s + 1], 16), 1.0, 0.0
        ).astype(BF16)
        for q in range(tiles):
            base = 16 * (s * tiles + q)
            mask_root[base : base + 16, :] = jnp.where(
                wide(label_tile[s : s + 1], 16) == q, 1.0, 0.0
            ).astype(BF16)

    old_pos = old + pos0 + [mass]
    at_head = [gather(v, head_tile, head_lane) for v in old_pos]
    at_tail = [gather(v, tail_tile, tail_lane) for v in old_pos]

    def scatter(rows):
        halves = [half for row in rows for half in split(row)]
        parts = []
        for s in range(bond_rows):
            mask = mask_tail[16 * s : 16 * s + 16, :]
            parts.append(jnp.concatenate(
                [wide(half[s : s + 1], 16).astype(BF16) * mask for half in halves], axis=0
            ))
        out = dot_nn(jnp.concatenate(parts, axis=1), hot_tail[...])
        return [out[32 * i : 32 * i + 16] + out[32 * i + 16 : 32 * i + 32] for i in range(len(rows))]

    def spread(rows):
        pulls = [bent[d] * row for row in rows for d in range(3)]
        sums = scatter(pulls)
        return [
            jnp.concatenate([p - t[:bond_rows], -t[bond_rows:slot_rows]], axis=0)
            for p, t in zip(pulls, sums)
        ]

    def meet(moves):
        return [
            mass_head * m[:bond_rows] - near_mass * gather(m, spot_tile, spot_lane) for m in moves
        ]

    def bend(vector):
        return bent[0] * vector[0] + bent[1] * vector[1] + bent[2] * vector[2]

    def to_slots(rows):
        count = -(-len(rows) // SUBS)
        for v in range(count * SUBS):
            stage[SUBS * v : SUBS * v + SUBS, :] = (
                rows[v] if v < len(rows) and rows[v] is not None else jnp.zeros((SUBS, LANES), F32)
            )
        parts = []
        for s in range(bond_rows):
            value = jnp.concatenate(
                [stage[pl.ds(SUBS * SUBS * c + s, SUBS, stride=SUBS), :] for c in range(count)], axis=0
            )
            high, low = split(value)
            both = jnp.concatenate([high, low], axis=0).astype(BF16)
            size = both.shape[0]
            pieces = []
            for q in range(tiles):
                base = 16 * (s * tiles + q)
                mask = mask_root[base : base + 16, :]
                pieces.append(both * jnp.concatenate([mask] * (size // 16), axis=0))
            parts.append(jnp.concatenate(pieces, axis=0))
        out = dot_nn(jnp.concatenate(parts, axis=1), hot_root[...])
        half = SUBS * count
        return [
            [
                out[2 * half * q + SUBS * c : 2 * half * q + SUBS * c + SUBS]
                + out[2 * half * q + half + SUBS * c : 2 * half * q + half + SUBS * c + SUBS]
                for c in range(count)
            ]
            for q in range(tiles)
        ]

    def to_bonds(slots, row):
        total = jnp.zeros((bond_rows, LANES), F32)
        for q in range(tiles):
            total = jnp.where(
                label_tile == q, lanes_at(wide(slots[q][row : row + 1], bond_rows), label_lane), total
            )
        return total

    flags = jnp.where(is_far, 1.0, 0.0)
    steps = [(k, d) for k in range(ORDER + 1) for d in range(3)]
    pad = 2 * SUBS - len(steps)
    step_dims = [d for _, d in steps] + [0] * pad
    step_terms = [k for k, _ in steps] + [ORDER + 1] * pad
    quad = [(g, a, b) for g in range(ORDER) for a, b in SYM]
    dims_at = [pick_rows(step_dims[SUBS * c : SUBS * c + SUBS]) for c in range(2)]
    terms_at = [pick_rows(step_terms[SUBS * c : SUBS * c + SUBS]) for c in range(2)]
    quads_at = [
        [pick_rows([x[i] + (3 if i == 0 else 0) for x in quad[SUBS * c : SUBS * c + SUBS]]) for i in range(3)]
        for c in range(len(quad) // SUBS)
    ]

    arrive(first)
    far = [transpose8(in0[0, SUBS * q : SUBS * q + SUBS, :]) for q in range(tiles)]
    at_tail = [jnp.where(is_far, to_bonds(far, g), v) for g, v in enumerate(at_tail)]
    bond_old = [at_head[d] - at_tail[d] for d in range(3)]
    bond_new = [at_head[3 + d] - at_tail[3 + d] for d in range(3)]
    mass_head, mass_tail = at_head[6], at_tail[6]
    length = jnp.maximum(
        jnp.sqrt(bond_old[0] * bond_old[0] + bond_old[1] * bond_old[1] + bond_old[2] * bond_old[2]), 0.5
    )
    direction = [b / length for b in bond_old]
    scale = 1.0 / jnp.sqrt(mass_head + mass_tail)
    bent = [scale * d for d in direction]
    near_mass = jnp.where(is_far, 0.0, mass_tail)
    right1 = scale * (
        direction[0] * bond_new[0] + direction[1] * bond_new[1] + direction[2] * bond_new[2] - length
    )

    terms, fars = [right1], [flags]
    term_moves, term_meets, far_moves, far_meets = [], [], [], []

    def advance():
        moves = spread([terms[-1], fars[-1]])
        meets = meet(moves)
        term_moves.append(moves[:3])
        far_moves.append(moves[3:])
        term_meets.append(meets[:3])
        far_meets.append(meets[3:])
        terms.append(terms[-1] - bend(meets[:3]))
        fars.append(fars[-1] - bend(meets[3:]))

    half = ORDER // 2
    for _ in range(half):
        advance()

    def at_far(values, k):
        return fars[max(0, k - half)] * values[min(k, half)]

    slots1 = to_slots(
        [bent[d] * flags for d in range(3)] + [flags] + [at_far(fars, k) for k in range(1, ORDER)]
        + [None] + [at_far(terms, k) for k in range(ORDER + 1)]
    )
    normal = [s[0] for s in slots1]

    def send_terms(values, out):
        for q in range(tiles):
            for c in range(2):
                product = subs_at(normal[q], dims_at[c]) * subs_at(values[q], terms_at[c])
                out[c, SUBS * q : SUBS * q + SUBS, :] = transpose8(product)

    send_terms([s[1] for s in slots1], out1)
    for q in range(tiles):
        for c, (gap, a, b) in enumerate(quads_at):
            product = subs_at(normal[q], a) * subs_at(normal[q], b) * subs_at(normal[q], gap)
            out1[2 + c, SUBS * q : SUBS * q + SUBS, :] = transpose8(product)
    second = copies(1, out1, in1, forth, True, False)

    for _ in range(ORDER - half):
        advance()
    last_moves = spread([terms[ORDER]])
    last_meets = meet(last_moves)
    upper = pick_rows([0] * 4 + [1] * 4)
    normal_a = [subs_at(n, upper) for n in normal]
    normal_b = [subs_at(n, pick_rows([2] * 8)) for n in normal]
    base1 = sum(terms[1:], terms[0])

    arrive(second)

    def collect(land):
        found = []
        for part in range(land.shape[0]):
            total = land[part, 0:SUBS, :]
            for q in range(1, tiles):
                total = total + land[part, SUBS * q : SUBS * q + SUBS, :]
            for shift in (4, 2, 1):
                total = total + pltpu.roll(total, shift, 0)
            for g in range(SUBS):
                found.append(lanes_at(total, entry + width * g))
        return found

    heavy = in0[0, hub_row : hub_row + 1, :] if hub_row != centre else out0[0, 0:1, :]
    mass_send = lanes_at(wide(heavy), entry + 6 * width)
    got = collect(in1)
    matrix = [
        {ab: -mass_send * got[2 * SUBS + 6 * g + i] for i, ab in enumerate(SYM)} for g in range(ORDER)
    ]

    def owner(got, out):
        moved = []
        for k in range(ORDER + 1):
            total = [-mass_send * got[3 * k + d] for d in range(3)]
            for i in range(k):
                push = matrix[k - 1 - i]
                for d in range(3):
                    for e in range(3):
                        total[d] = total[d] + push[(min(d, e), max(d, e))] * moved[i][e]
            moved.append(total)
        for c in range(2):
            message = jnp.zeros((SUBS, LANES), F32)
            for g in range(SUBS):
                v = SUBS * c + g
                if v < 3 * ORDER:
                    value = moved[v % ORDER][v // ORDER]
                elif v < 3 * ORDER + 3:
                    value = sum([m[v - 3 * ORDER] for m in moved[1:]], moved[0][v - 3 * ORDER])
                else:
                    continue
                message = jnp.where(group == g, value, message)
            out[c] = message

    owner(got, out2)
    third = copies(2, out2, in2, back, False, True)

    weights, weight_moves, weight_meets = [], [], []
    for k in range(ORDER):
        if k == 0:
            weights.append(fars[0])
            weight_moves.append(far_moves[0])
            weight_meets.append(far_meets[0])
        else:
            weights.append(weights[-1] + fars[k])
            weight_moves.append([a + b for a, b in zip(weight_moves[-1], far_moves[k])])
            weight_meets.append([a + b for a, b in zip(weight_meets[-1], far_meets[k])])
    base_moves = [sum([m[d] for m in term_moves], last_moves[d]) for d in range(3)]
    base_meets = [sum([m[d] for m in term_meets], last_meets[d]) for d in range(3)]

    def answers(land):
        low = [transpose8(land[0, SUBS * q : SUBS * q + SUBS, :]) for q in range(tiles)]
        high = [transpose8(land[1, SUBS * q : SUBS * q + SUBS, :]) for q in range(tiles)]
        replies = []
        for q in range(tiles):
            product = low[q] * normal_a[q]
            replies.append(product + pltpu.roll(product, 4, 0) + high[q] * normal_b[q])
        return [to_bonds(replies, k) for k in range(ORDER)], high

    def through(weights, injected):
        total = weights[0] * injected[ORDER - 1]
        for k in range(1, ORDER):
            total = total + weights[k] * injected[ORDER - 1 - k]
        return total

    arrive(third)
    injected1, high = answers(in2)
    tail_moves = [to_bonds(high, 4 + d) for d in range(3)]
    sol1 = base1 + through(weights, injected1)
    stretch = [
        bond_new[d]
        - (base_meets[d] + through([w[d] for w in weight_meets], injected1) - flags * tail_moves[d])
        for d in range(3)
    ]
    current = stretch[0] * stretch[0] + stretch[1] * stretch[1] + stretch[2] * stretch[2]
    square = length * length
    goal = jnp.sqrt(jnp.maximum(2.0 * square - current, 0.5 * square))
    right2 = scale * (length - goal)
    slots3 = to_slots([fars[k] * right2 for k in range(ORDER + 1)])
    send_terms([s[0] for s in slots3], out3)
    fourth = copies(3, out3, in3, forth, True, False)

    term, both = right2, sol1 + right2
    for k in range(ORDER + 1):
        moves = spread([term])
        base_moves = [a + b for a, b in zip(base_moves, moves)]
        if k < ORDER:
            term = term - bend(meet(moves))
            both = both + term
        if k == 1:
            arrive(fourth)
            owner(collect(in3), out4)
            fifth = copies(4, out4, in4, back, False, True)

    place_tile = lax.shift_right_logical(place_of[:atom_rows], 7)
    place_lane = place_of[:atom_rows] & (LANES - 1)
    number = lax.broadcasted_iota(I32, (atom_rows, LANES), 0) * LANES + lax.broadcasted_iota(
        I32, (atom_rows, LANES), 1
    )
    entry_of = jnp.full((atom_rows, LANES), -1, I32)
    for e in range(send_count):
        entry_of = jnp.where(number == wide(send_rep[0:1, e : e + 1] + jnp.zeros((1, LANES), I32), atom_rows), e, entry_of)
    sent = entry_of >= 0
    entry_of = jnp.maximum(entry_of, 0)

    arrive(fifth)
    injected2, _ = answers(in4)
    both = both + through(weights, injected2)
    mult_ref[0, 0] = both.reshape(1, bonds)
    injected = [a + b for a, b in zip(injected1, injected2)]
    own = wide(in2[1, centre : centre + 1, :] + in4[1, centre : centre + 1, :], atom_rows)
    for d in range(3):
        total = jnp.concatenate(
            [
                base_moves[d][:bond_rows]
                + through([w[d][:bond_rows] for w in weight_moves], injected),
                base_moves[d][bond_rows:],
            ],
            axis=0,
        )
        result = pos0[d] - mass * gather(total, place_tile, place_lane)
        result = result - jnp.where(sent, lanes_at(own, entry_of + width * (4 + d)), 0.0)
        pos_ref[d, 0, 0] = result.reshape(1, atoms)
    for copy in pending:
        copy.wait_send()


def per_device(axes, sizes, old_pos, displacement, inv_mass, bond_head, bond_tail, send_list):
    atoms, bonds, send_count = old_pos.shape[-1], bond_head.shape[-1], send_list.shape[-1]
    rows = 4 * SUBS
    vmem = lambda *shape: pltpu.VMEM(shape + (LANES,), F32)
    half = lambda *shape: pltpu.VMEM(shape, BF16)
    bond_rows = bonds // LANES
    return pl.pallas_call(
        functools.partial(kernel, axes, sizes, send_count),
        out_shape=(
            jax.ShapeDtypeStruct(old_pos.shape, F32),
            jax.ShapeDtypeStruct(bond_head.shape, F32),
        ),
        in_specs=[pl.BlockSpec(memory_space=pltpu.VMEM)] * 6,
        out_specs=(pl.BlockSpec(memory_space=pltpu.VMEM), pl.BlockSpec(memory_space=pltpu.VMEM)),
        scratch_shapes=[
            vmem(atoms // LANES * SUBS),
            half(LANES, bonds), half(bonds, LANES), half(bonds, LANES),
            half(16 * bond_rows, LANES), half(16 * bond_rows * 4, LANES),
            vmem(2 * SUBS * SUBS),
            vmem(1, SUBS), vmem(1, rows),
            vmem(5, rows), vmem(5, rows),
            vmem(2, SUBS), vmem(2, rows),
            vmem(2, rows), vmem(2, rows),
            vmem(2, SUBS), vmem(2, rows),
            pltpu.SemaphoreType.DMA((5, 27)),
            pltpu.SemaphoreType.DMA((5, 27)),
        ],
        compiler_params=pltpu.CompilerParams(
            collective_id=0, has_side_effects=True, vmem_limit_bytes=56 * 1024 * 1024
        ),
    )(old_pos, displacement, inv_mass, bond_head, bond_tail, send_list)


def solution(mesh):
    axes = ("gx", "gy", "gz")
    sizes = tuple(mesh.shape[name] for name in axes)
    return jax.shard_map(
        functools.partial(per_device, axes, sizes),
        mesh=mesh,
        in_specs=(
            P(None, "gx", "gy", "gz", None),
            P(None, "gx", "gy", "gz", None),
            P("gx", "gy", "gz", None),
            P("gx", "gy", "gz", None),
            P("gx", "gy", "gz", None),
            P("gx", "gy", "gz", None),
        ),
        out_specs=(P(None, "gx", "gy", "gz", None), P("gx", "gy", "gz", None)),
        check_vma=False,
    )
```

```python
import functools

import jax
import jax.numpy as jnp
from jax import lax
from jax.experimental import pallas as pl
from jax.experimental.pallas import tpu as pltpu
from jax.sharding import PartitionSpec as P

ORDER = 4
LANES = 128
SUBS = 8
F32, BF16, I32 = jnp.float32, jnp.bfloat16, jnp.int32
MESH = pl.DeviceIdType.MESH
SYM = ((0, 0), (0, 1), (0, 2), (1, 1), (1, 2), (2, 2))


def dot_nt(left, right):
    return lax.dot_general(left, right, (((1,), (1,)), ((), ())), preferred_element_type=F32)


def dot_nn(left, right):
    return lax.dot_general(left, right, (((1,), (0,)), ((), ())), preferred_element_type=F32)


def wide(row, count=SUBS):
    return jnp.broadcast_to(row, (count, row.shape[1]))


def lanes_at(rows, index):
    return jnp.take_along_axis(rows, index, axis=1, mode="promise_in_bounds")


def subs_at(rows, index):
    return jnp.take_along_axis(rows, index, axis=0, mode="promise_in_bounds")


def split(value):
    high = value.astype(BF16).astype(F32)
    return high, value - high


def flips(n):
    return n >= 4 and n % 2 == 0


def routes(sizes):
    plane = [(a, c) for a in range(3) for c in range(3)]
    classes = [(a, b, c) for b in (0, 2, 1) for a, c in plane[:SUBS]]
    classes += [plane[SUBS][:1] + (b,) + plane[SUBS][1:] for b in (0, 2, 1)]
    direct, forth, back = [], [], []
    for cls in classes:
        direct.append(tuple((1 - c) for c in cls))
        forth.append(tuple((0, 1, -2)[c] if flips(n) else c - 1 for c, n in zip(cls, sizes)))
        back.append(tuple((0, 1, 2)[c] if flips(n) else 1 - c for c, n in zip(cls, sizes)))
    return classes, direct, forth, back


def kernel(
    axes, sizes, send_count,
    old_hbm, move_hbm, mass_hbm, head_hbm, tail_hbm, send_hbm,
    pos_ref, mult_ref,
    old_ref, move_ref, mass_ref, head_ref, tail_ref, send_ref, load_sem,
    table, hot_head, hot_tail, hot_root, mask_tail, mask_root, stage,
    out0, in0, out1, in1, out2, in2, out3, in3, out4, in4,
    send_sem, recv_sem,
):
    atoms, bonds = old_ref.shape[-1], head_ref.shape[-1]
    atom_rows, bond_rows = atoms // LANES, bonds // LANES
    slot_rows = bond_rows + -(-(atoms - bonds) // LANES)
    width = send_count
    bits = width.bit_length() - 1
    classes, direct, forth, back = routes(sizes)
    centre = classes.index((1, 1, 1))
    hub_row = classes.index(tuple(0 if flips(n) else 1 for n in sizes))
    tiles = -(-len(classes) // SUBS)
    here = [lax.axis_index(name) for name in axes]
    turn = [1 - 2 * lax.rem(i, 2) if flips(n) else 1 for i, n in zip(here, sizes)]

    twin = sizes[1] == 2

    def nowhere(offset):
        return all(o % n == 0 for o, n in zip(offset, sizes))

    def target(offset):
        return tuple(
            lax.rem(i + o * s + 2 * n, n) for i, o, s, n in zip(here, offset, turn, sizes)
        )

    greet = []
    for group in (direct, forth, back):
        for offset in group:
            key = tuple(o % n for o, n in zip(offset, sizes))
            if any(key) and key not in [k for k, _ in greet]:
                greet.append((key, offset))
    loads = [
        pltpu.make_async_copy(source, dest, load_sem.at[i])
        for i, (source, dest) in enumerate((
            (send_hbm, send_ref), (old_hbm, old_ref), (move_hbm, move_ref), (mass_hbm, mass_ref),
            (head_hbm, head_ref), (tail_hbm, tail_ref),
        ))
    ]
    for load in loads:
        load.start()
    barrier = pltpu.get_barrier_semaphore()
    for _, offset in greet:
        pl.semaphore_signal(barrier, inc=1, device_id=target(offset), device_id_type=MESH)

    sub = lax.broadcasted_iota(I32, (SUBS, LANES), 0)
    lane = lax.broadcasted_iota(I32, (SUBS, LANES), 1)
    group = lax.shift_right_logical(lane, bits)
    entry = lane & (width - 1)
    swap = (group - sub) & (SUBS - 1)
    unskew = (lane + width * sub) & (LANES - 1)

    def transpose8(x):
        x = pltpu.roll(x, 0, 1, stride=width, stride_axis=0)
        return lanes_at(subs_at(x, swap), unskew)

    for load in loads:
        load.wait()

    old = [old_ref[k, 0, 0].reshape(atom_rows, LANES) for k in range(3)]
    pos0 = [old[k] + move_ref[k, 0, 0].reshape(atom_rows, LANES) for k in range(3)]
    mass = mass_ref[0, 0].reshape(atom_rows, LANES)
    values = old + pos0 + [mass, jnp.zeros((atom_rows, LANES), F32)]
    for g, value in enumerate(values):
        for q in range(atom_rows):
            table[SUBS * q + g : SUBS * q + g + 1, :] = value[q : q + 1]
    send_row = jnp.concatenate(
        [send_ref[0, 0], jnp.zeros((1, LANES - send_count), I32)], axis=1
    )
    send_rep = lanes_at(wide(send_row), entry)
    send_tile, send_lane = lax.shift_right_logical(send_rep, 7), send_rep & (LANES - 1)
    found = jnp.zeros((SUBS, LANES), F32)
    for q in range(atom_rows):
        found = jnp.where(
            send_tile == q, lanes_at(table[SUBS * q : SUBS * q + SUBS, :], send_lane), found
        )
    found = jnp.sum(jnp.where(group == sub, found, 0.0), axis=0, keepdims=True)
    out0[0] = wide(found)
    for land in (in1, in3):
        for part in range(land.shape[0]):
            land[part, centre : centre + 1, :] = jnp.zeros((1, LANES), F32)
            land[part, len(classes) :, :] = jnp.zeros((SUBS * tiles - len(classes), LANES), F32)
            if twin:
                land[part, 3 * SUBS + 1 : 3 * SUBS + 2, :] = jnp.zeros((1, LANES), F32)
    head = head_ref[0, 0].reshape(bond_rows, LANES)
    tail = tail_ref[0, 0].reshape(bond_rows, LANES)
    head_tile, head_lane = lax.shift_right_logical(head, 7), head & (LANES - 1)
    tail_tile, tail_lane = lax.shift_right_logical(tail, 7), tail & (LANES - 1)
    is_far = tail >= atoms
    slot = jnp.maximum(tail - atoms, 0)
    block = lax.shift_right_logical(slot, bits)
    one = lambda test: jnp.where(test, 1, 0)
    bx = one(block >= 9) + one(block >= 18)
    rest = block - 9 * bx
    by = one(rest >= 3) + one(rest >= 6)
    bz = rest - 3 * by
    place = [
        1 - s * (b - 1) if flips(n) else b
        for b, s, n in zip((bx, by, bz), turn, sizes)
    ]
    across_plane = place[0] * 3 + place[2]
    level = jnp.where(place[1] == 0, 0, 3 - place[1])
    slot_row = jnp.where(across_plane < SUBS, SUBS * level + across_plane, 3 * SUBS + level)
    slot = slot_row * width + (slot & (width - 1))

    def gather(rows, tile, index, start=0.0, count=None):
        shape = index.shape
        total = jnp.full(shape, start, rows.dtype)
        for q in range(count or rows.shape[0]):
            total = jnp.where(tile == q, lanes_at(wide(rows[q : q + 1], shape[0]), index), total)
        return total

    deep = lax.broadcasted_iota(I32, (LANES, LANES), 0)
    across = lax.broadcasted_iota(I32, (LANES, LANES), 1)
    row16 = lax.broadcasted_iota(I32, (2 * SUBS, LANES), 0)
    parts = []
    for s in range(bond_rows):
        hot_head[:, s * LANES : (s + 1) * LANES] = jnp.where(
            deep == wide(head_lane[s : s + 1], LANES), 1.0, 0.0
        ).astype(BF16)
        number = lane[0:1] + (s * LANES + 1)
        high = (number - (number & 7)).astype(F32)
        low = (number & 7).astype(F32)
        match = row16 == wide(head_tile[s : s + 1], 2 * SUBS)
        parts.append(jnp.concatenate(
            [jnp.where(match, wide(high, 16), 0.0), jnp.where(match, wide(low, 16), 0.0)], axis=0
        ).astype(BF16))
    owner_of = dot_nt(jnp.concatenate(parts, axis=1), hot_head[...])
    owner_of = owner_of[:16] + owner_of[16:]
    free = jnp.where(owner_of == 0.0, 1.0, 0.0).astype(BF16)
    before = dot_nn(free, jnp.where(deep < across, 1.0, 0.0).astype(BF16))
    totals = dot_nn(free, jnp.ones((LANES, LANES), BF16))
    for q in range(atom_rows - 1):
        before = before + jnp.where(row16 > q, wide(totals[q : q + 1], 16), 0.0)
    place_of = jnp.where(owner_of > 0.0, owner_of - 1.0, before + float(bonds)).astype(I32)
    spot = gather(place_of, tail_tile, tail_lane, 0, atom_rows)
    spot = jnp.where(is_far, -1, spot)
    spot_tile, spot_lane = lax.shift_right_arithmetic(spot, 7), spot & (LANES - 1)

    label = jnp.where(is_far, slot, -1)
    for _ in range(ORDER + 1):
        label = jnp.where(is_far, slot, gather(label, spot_tile, spot_lane, -1))
    label_tile, label_lane = lax.shift_right_arithmetic(label, 7), label & (LANES - 1)

    def columns(index, dest):
        col = index.astype(F32).T
        line = lane[0:1].astype(F32)
        for s in range(bond_rows):
            dest[s * LANES : (s + 1) * LANES, :] = jnp.where(
                col[:, s : s + 1] == line, 1.0, 0.0
            ).astype(BF16)

    columns(spot_lane, hot_tail)
    columns(label_lane, hot_root)
    for s in range(bond_rows):
        mask_tail[16 * s : 16 * s + 16, :] = jnp.where(
            row16 == wide(spot_tile[s : s + 1], 16), 1.0, 0.0
        ).astype(BF16)
        for q in range(tiles):
            base = 16 * (s * tiles + q)
            mask_root[base : base + 16, :] = jnp.where(
                wide(label_tile[s : s + 1], 16) == q, 1.0, 0.0
            ).astype(BF16)

    old_pos = old + pos0 + [mass]
    at_head = [gather(v, head_tile, head_lane) for v in old_pos]
    at_tail = [gather(v, tail_tile, tail_lane) for v in old_pos]

    def scatter(rows):
        halves = [half for row in rows for half in split(row)]
        parts = []
        for s in range(bond_rows):
            mask = mask_tail[16 * s : 16 * s + 16, :]
            parts.append(jnp.concatenate(
                [wide(half[s : s + 1], 16).astype(BF16) * mask for half in halves], axis=0
            ))
        out = dot_nn(jnp.concatenate(parts, axis=1), hot_tail[...])
        return [out[32 * i : 32 * i + 16] + out[32 * i + 16 : 32 * i + 32] for i in range(len(rows))]

    def spread(bent, rows):
        pulls = [bent[d] * row for row in rows for d in range(3)]
        sums = scatter(pulls)
        return [
            jnp.concatenate([p - t[:bond_rows], -t[bond_rows:slot_rows]], axis=0)
            for p, t in zip(pulls, sums)
        ], sums

    def meet(moves):
        return [
            mass_head * m[:bond_rows] - near_mass * gather(m, spot_tile, spot_lane) for m in moves
        ]

    def bend(bent, vector):
        return bent[0] * vector[0] + bent[1] * vector[1] + bent[2] * vector[2]

    def to_slots(rows):
        count = -(-len(rows) // SUBS)
        for v in range(count * SUBS):
            stage[SUBS * v : SUBS * v + SUBS, :] = (
                rows[v] if v < len(rows) and rows[v] is not None else jnp.zeros((SUBS, LANES), F32)
            )
        parts = []
        for s in range(bond_rows):
            value = jnp.concatenate(
                [stage[pl.ds(SUBS * SUBS * c + s, SUBS, stride=SUBS), :] for c in range(count)], axis=0
            )
            high, low = split(value)
            both = jnp.concatenate([high, low], axis=0).astype(BF16)
            size = both.shape[0]
            pieces = []
            for q in range(tiles):
                base = 16 * (s * tiles + q)
                mask = mask_root[base : base + 16, :]
                pieces.append(both * jnp.concatenate([mask] * (size // 16), axis=0))
            parts.append(jnp.concatenate(pieces, axis=0))
        out = dot_nn(jnp.concatenate(parts, axis=1), hot_root[...])
        half = SUBS * count
        return [
            [
                out[2 * half * q + SUBS * c : 2 * half * q + SUBS * c + SUBS]
                + out[2 * half * q + half + SUBS * c : 2 * half * q + half + SUBS * c + SUBS]
                for c in range(count)
            ]
            for q in range(tiles)
        ]

    def to_bonds(slots, row):
        total = jnp.zeros((bond_rows, LANES), F32)
        for q in range(tiles):
            total = jnp.where(
                label_tile == q, lanes_at(wide(slots[q][row : row + 1], bond_rows), label_lane), total
            )
        return total

    flags = jnp.where(is_far, 1.0, 0.0)
    slot_tile, slot_lane = lax.shift_right_logical(slot, 7), slot & (LANES - 1)
    parts = []
    for s in range(bond_rows):
        number = lane[0:1] + (s * LANES + 1)
        high = (number - (number & 7)).astype(F32)
        low = (number & 7).astype(F32)
        match = jnp.where(is_far[s : s + 1], slot_tile[s : s + 1], -1)
        match = row16 == wide(match, 2 * SUBS)
        parts.append(jnp.concatenate(
            [jnp.where(match, wide(high, 16), 0.0), jnp.where(match, wide(low, 16), 0.0)], axis=0
        ).astype(BF16))
    bond_of = dot_nn(jnp.concatenate(parts, axis=1), hot_root[...])
    bond_of = (bond_of[:SUBS] + bond_of[16 : 16 + SUBS]).astype(I32) - 1
    bond_tile, bond_lane = lax.shift_right_arithmetic(bond_of, 7), bond_of & (LANES - 1)


    order = sorted(range(len(classes)), key=lambda r: -(classes[r][0] + classes[r][2]))

    def copies(step, source, landing, offsets, each, whole):
        started = []
        for row in order:
            if row == centre and not whole or twin and classes[row][1] == 2:
                continue
            line = row if each else 0
            if nowhere(offsets[row]):
                landing[:, row : row + 1, :] = source[:, line : line + 1, :]
                continue
            copy = pltpu.make_async_remote_copy(
                source.at[:, line], landing.at[:, row],
                send_sem.at[step, row], recv_sem.at[step, row],
                device_id=target(offsets[row]), device_id_type=MESH,
            )
            copy.start()
            started.append(copy)
        return started

    def post(out, part, value):
        pieces = [value[SUBS * q : SUBS * q + SUBS] for q in range(tiles)]
        if twin:
            pieces[0] = pieces[0] + pieces[1]
            pieces[3] = pieces[3] + jnp.where(sub == 0, wide(pieces[3][1:2]), 0.0)
        for q in range(tiles):
            if not (twin and q == 1):
                out[part, SUBS * q : SUBS * q + SUBS, :] = pieces[q]

    def landed(land, part):
        parts = [land[part, SUBS * q : SUBS * q + SUBS, :] for q in range(tiles)]
        if twin:
            parts[1] = parts[0]
            parts[3] = jnp.where(sub == 1, wide(parts[3][0:1]), parts[3])
        return parts

    pending = []

    def arrive(started):
        for copy in started:
            copy.wait_recv()
        pending.extend(started)

    pl.semaphore_wait(barrier, len(greet))
    first = copies(0, out0, in0, direct, False, False)

    mass_head = at_head[6]

    def geometry(head_data, tail_data):
        olds = [head_data[d] - tail_data[d] for d in range(3)]
        news = [head_data[3 + d] - tail_data[3 + d] for d in range(3)]
        size = jnp.maximum(jnp.sqrt(olds[0] * olds[0] + olds[1] * olds[1] + olds[2] * olds[2]), 0.5)
        direction = [b / size for b in olds]
        scale = 1.0 / jnp.sqrt(head_data[6] + tail_data[6])
        right = scale * (
            direction[0] * news[0] + direction[1] * news[1] + direction[2] * news[2] - size
        )
        return news, size, scale, [scale * d for d in direction], right

    _, _, _, bent, right = geometry(at_head, at_tail)
    bent = [jnp.where(is_far, 0.0, b) for b in bent]
    near_mass = jnp.where(is_far, 0.0, at_tail[6])
    kids = gather(flags, spot_tile, spot_lane) * near_mass
    series = [jnp.where(is_far, 0.0, right)] + [kids * b for b in bent]
    drive, square_of = [], []
    for k in range(ORDER):
        if k == ORDER - 1:
            series = series[:1]
        moves, sums = spread(bent, series)
        drive.append([mass_head * sums[d][:bond_rows] * flags for d in range(3)])
        if k < ORDER - 1:
            square_of.append(
                [mass_head * sums[3 + 3 * b + a][:bond_rows] * flags for a, b in SYM]
            )
            if k == ORDER - 2:
                series, moves = series[:1], moves[:3]
            meets = meet(moves)
            series = [
                v - bend(bent, meets[3 * i : 3 * i + 3]) for i, v in enumerate(series)
            ]

    spread_lane = width * sub + entry

    def to_rows(packed, row):
        return jnp.concatenate(
            [lanes_at(wide(packed[q][row : row + 1]), spread_lane) for q in range(tiles)], axis=0
        )

    def from_bonds(value):
        rows = gather(value, bond_tile, bond_lane)
        return to_rows([rows[q : q + 1] for q in range(tiles)], 0)

    used = from_bonds(jnp.ones((bond_rows, LANES), F32)) > 0.0
    head_rows = [from_bonds(v) for v in at_head]
    flat = [v for group in drive + square_of for v in group]
    flat = to_slots(flat)
    flat = [
        to_rows([part[v // SUBS] for part in flat], v % SUBS) for v in range(3 * ORDER + 6 * (ORDER - 1))
    ]
    drive = [flat[3 * k : 3 * k + 3] for k in range(ORDER)]
    square_of = [flat[3 * ORDER + 6 * k : 3 * ORDER + 6 * k + 6] for k in range(ORDER - 1)]
    entry_rows = jnp.concatenate([entry] * tiles, axis=0)
    group_rows = jnp.concatenate([group] * tiles, axis=0)

    arrive(first)
    landing = jnp.concatenate(landed(in0, 0), axis=0)
    tail_rows = [lanes_at(landing, entry_rows + width * g) for g in range(7)]
    _, _, _, normal, start = geometry(head_rows, tail_rows)
    normal = [jnp.where(used, b, 0.0) for b in normal]
    pairs = [normal[a] * normal[b] for a, b in SYM]
    keep = 1.0 - head_rows[6] * (pairs[0] + pairs[3] + pairs[5])
    pushes = [
        q[0] * pairs[0] + q[3] * pairs[3] + q[5] * pairs[5]
        + 2.0 * (q[1] * pairs[1] + q[2] * pairs[2] + q[4] * pairs[4])
        for q in square_of
    ]
    chain, reply = [start], [None, keep]
    for k in range(1, ORDER + 1):
        value = keep * chain[-1] + (
            normal[0] * drive[k - 1][0] + normal[1] * drive[k - 1][1] + normal[2] * drive[k - 1][2]
        )
        for i in range(k - 1):
            value = value + pushes[k - 2 - i] * chain[i]
        chain.append(value)
    for k in range(2, ORDER):
        value = keep * reply[-1] + pushes[k - 2]
        for i in range(1, k - 1):
            value = value + pushes[k - 2 - i] * reply[i]
        reply.append(value)

    def packed(values):
        total = jnp.zeros((SUBS * tiles, LANES), F32)
        for g, value in enumerate(values):
            total = jnp.where(group_rows == g, value, total)
        return total

    def post_terms(values, out):
        steps = [normal[d] * values[k] for k in range(ORDER + 1) for d in range(3)]
        post(out, 0, packed(steps[:SUBS]))
        post(out, 1, packed(steps[SUBS:]))

    post_terms(chain, out1)
    quads = [p if reply[g] is None else reply[g] * p for g in range(ORDER) for p in pairs]
    for c in range(len(quads) // SUBS):
        post(out1, 2 + c, packed(quads[SUBS * c : SUBS * c + SUBS]))
    second = copies(1, out1, in1, forth, True, False)

    low = packed([normal[0]] * 4 + [normal[1]] * 4)
    normal_a = [transpose8(low[SUBS * q : SUBS * q + SUBS]) for q in range(tiles)]
    normal_b = [
        transpose8(normal[2][SUBS * q : SUBS * q + SUBS]) for q in range(tiles)
    ]
    far = [transpose8(piece) for piece in landed(in0, 0)]
    at_tail = [jnp.where(is_far, to_bonds(far, g), v) for g, v in enumerate(at_tail)]
    bond_new, length, scale, bent, right1 = geometry(at_head, at_tail)

    terms, fars = [right1], [flags]
    term_moves, term_meets, far_moves, far_meets = [], [], [], []

    def advance():
        moves, _ = spread(bent, [terms[-1], fars[-1]])
        meets = meet(moves)
        term_moves.append(moves[:3])
        far_moves.append(moves[3:])
        term_meets.append(meets[:3])
        far_meets.append(meets[3:])
        terms.append(terms[-1] - bend(bent, meets[:3]))
        fars.append(fars[-1] - bend(bent, meets[3:]))

    for _ in range(ORDER):
        advance()
    last_moves, _ = spread(bent, [terms[ORDER]])
    last_meets = meet(last_moves)
    base1 = sum(terms[1:], terms[0])

    arrive(second)

    def collect(land):
        found = []
        for part in range(land.shape[0]):
            total = land[part, 0:SUBS, :]
            for q in range(1, tiles):
                if not (twin and q == 1):
                    total = total + land[part, SUBS * q : SUBS * q + SUBS, :]
            for shift in (4, 2, 1):
                total = total + pltpu.roll(total, shift, 0)
            for g in range(SUBS):
                found.append(lanes_at(total, entry + width * g))
        return found

    heavy = in0[0, hub_row : hub_row + 1, :] if hub_row != centre else out0[0, 0:1, :]
    mass_send = lanes_at(wide(heavy), entry + 6 * width)
    got = collect(in1)
    matrix = [
        {ab: -mass_send * got[2 * SUBS + 6 * g + i] for i, ab in enumerate(SYM)} for g in range(ORDER)
    ]

    def owner(got, out):
        moved = []
        for k in range(ORDER + 1):
            total = [-mass_send * got[3 * k + d] for d in range(3)]
            for i in range(k):
                push = matrix[k - 1 - i]
                for d in range(3):
                    for e in range(3):
                        total[d] = total[d] + push[(min(d, e), max(d, e))] * moved[i][e]
            moved.append(total)
        for c in range(2):
            message = jnp.zeros((SUBS, LANES), F32)
            for g in range(SUBS):
                v = SUBS * c + g
                if v < 3 * ORDER:
                    value = moved[v % ORDER][v // ORDER]
                elif v < 3 * ORDER + 3:
                    value = sum([m[v - 3 * ORDER] for m in moved[1:]], moved[0][v - 3 * ORDER])
                else:
                    continue
                message = jnp.where(group == g, value, message)
            out[c] = message

    owner(got, out2)
    third = copies(2, out2, in2, back, False, True)

    weights, weight_moves, weight_meets = [], [], []
    for k in range(ORDER):
        if k == 0:
            weights.append(fars[0])
            weight_moves.append(far_moves[0])
            weight_meets.append(far_meets[0])
        else:
            weights.append(weights[-1] + fars[k])
            weight_moves.append([a + b for a, b in zip(weight_moves[-1], far_moves[k])])
            weight_meets.append([a + b for a, b in zip(weight_meets[-1], far_meets[k])])
    base_moves = [sum([m[d] for m in term_moves], last_moves[d]) for d in range(3)]
    base_meets = [sum([m[d] for m in term_meets], last_meets[d]) for d in range(3)]

    def answers(land):
        low = [transpose8(piece) for piece in landed(land, 0)]
        high = [transpose8(piece) for piece in landed(land, 1)]
        replies = []
        for q in range(tiles):
            product = low[q] * normal_a[q]
            replies.append(product + pltpu.roll(product, 4, 0) + high[q] * normal_b[q])
        return replies, high

    def through(weights, injected):
        total = weights[0] * injected[ORDER - 1]
        for k in range(1, ORDER):
            total = total + weights[k] * injected[ORDER - 1 - k]
        return total

    arrive(third)
    replies1, high = answers(in2)
    injected1 = [to_bonds(replies1, k) for k in range(ORDER)]
    tail_moves = [to_bonds(high, 4 + d) for d in range(3)]
    sol1 = base1 + through(weights, injected1)
    stretch = [
        bond_new[d]
        - (base_meets[d] + through([w[d] for w in weight_meets], injected1) - flags * tail_moves[d])
        for d in range(3)
    ]
    current = stretch[0] * stretch[0] + stretch[1] * stretch[1] + stretch[2] * stretch[2]
    square = length * length
    goal = jnp.sqrt(jnp.maximum(2.0 * square - current, 0.5 * square))
    right2 = scale * (length - goal)
    slots3 = to_slots([fars[k] * right2 for k in range(ORDER + 1)])
    slots3 = [part[0] for part in slots3]
    post_terms([to_rows(slots3, k) for k in range(ORDER + 1)], out3)
    fourth = copies(3, out3, in3, forth, True, False)

    term, both = right2, sol1 + right2
    for k in range(ORDER + 1):
        moves, _ = spread(bent, [term])
        base_moves = [a + b for a, b in zip(base_moves, moves)]
        if k < ORDER:
            term = term - bend(bent, meet(moves))
            both = both + term
        if k == 1:
            arrive(fourth)
            owner(collect(in3), out4)
            fifth = copies(4, out4, in4, back, False, True)

    place_tile = lax.shift_right_logical(place_of[:atom_rows], 7)
    place_lane = place_of[:atom_rows] & (LANES - 1)
    number = lax.broadcasted_iota(I32, (atom_rows, LANES), 0) * LANES + lax.broadcasted_iota(
        I32, (atom_rows, LANES), 1
    )
    entry_of = jnp.full((atom_rows, LANES), -1, I32)
    for e in range(send_count):
        entry_of = jnp.where(number == wide(send_rep[0:1, e : e + 1] + jnp.zeros((1, LANES), I32), atom_rows), e, entry_of)
    sent = entry_of >= 0
    entry_of = jnp.maximum(entry_of, 0)

    atom_label = jnp.where(
        place_tile < bond_rows, gather(label, place_tile, place_lane, -1, bond_rows), -1
    )
    atom_tile, atom_lane = lax.shift_right_arithmetic(atom_label, 7), atom_label & (LANES - 1)
    at_atoms = [pos0[d] - mass * gather(base_moves[d], place_tile, place_lane) for d in range(3)]
    weight_moves = [
        [mass * gather(w[d][:bond_rows], place_tile, place_lane) for d in range(3)]
        for w in weight_moves
    ]
    early = len(pending)
    for copy in pending:
        copy.wait_send()

    arrive(fifth)
    replies2, _ = answers(in4)
    both = both + through(weights, [to_bonds(replies2, k) for k in range(ORDER)])
    mult_ref[0, 0] = both.reshape(1, bonds)
    replies = [a + b for a, b in zip(replies1, replies2)]
    injected = []
    for k in range(ORDER):
        total = jnp.zeros((atom_rows, LANES), F32)
        for q in range(tiles):
            total = jnp.where(
                atom_tile == q, lanes_at(wide(replies[q][k : k + 1], atom_rows), atom_lane), total
            )
        injected.append(total)
    own = wide(in2[1, centre : centre + 1, :] + in4[1, centre : centre + 1, :], atom_rows)
    for d in range(3):
        result = at_atoms[d] - through([w[d] for w in weight_moves], injected)
        result = result - jnp.where(sent, lanes_at(own, entry_of + width * (4 + d)), 0.0)
        pos_ref[d, 0, 0] = result.reshape(1, atoms)
    for copy in pending[early:]:
        copy.wait_send()


def per_device(axes, sizes, old_pos, displacement, inv_mass, bond_head, bond_tail, send_list):
    atoms, bonds, send_count = old_pos.shape[-1], bond_head.shape[-1], send_list.shape[-1]
    rows = 4 * SUBS
    vmem = lambda *shape: pltpu.VMEM(shape + (LANES,), F32)
    half = lambda *shape: pltpu.VMEM(shape, BF16)
    bond_rows = bonds // LANES
    return pl.pallas_call(
        functools.partial(kernel, axes, sizes, send_count),
        out_shape=(
            pltpu.VMEM(old_pos.shape, F32),
            pltpu.VMEM(bond_head.shape, F32),
        ),
        in_specs=[pl.BlockSpec(memory_space=pltpu.HBM)] * 6,
        out_specs=(pl.BlockSpec(memory_space=pltpu.VMEM), pl.BlockSpec(memory_space=pltpu.VMEM)),
        scratch_shapes=[
            pltpu.VMEM(old_pos.shape, F32), pltpu.VMEM(displacement.shape, F32),
            pltpu.VMEM(inv_mass.shape, F32), pltpu.VMEM(bond_head.shape, I32),
            pltpu.VMEM(bond_tail.shape, I32), pltpu.VMEM(send_list.shape, I32),
            pltpu.SemaphoreType.DMA((6,)),
            vmem(atoms // LANES * SUBS),
            half(LANES, bonds), half(bonds, LANES), half(bonds, LANES),
            half(16 * bond_rows, LANES), half(16 * bond_rows * 4, LANES),
            vmem(4 * SUBS * SUBS),
            vmem(1, SUBS), vmem(1, rows),
            vmem(5, rows), vmem(5, rows),
            vmem(2, SUBS), vmem(2, rows),
            vmem(2, rows), vmem(2, rows),
            vmem(2, SUBS), vmem(2, rows),
            pltpu.SemaphoreType.DMA((5, 27)),
            pltpu.SemaphoreType.DMA((5, 27)),
        ],
        compiler_params=pltpu.CompilerParams(
            collective_id=0, has_side_effects=True, vmem_limit_bytes=56 * 1024 * 1024
        ),
    )(old_pos, displacement, inv_mass, bond_head, bond_tail, send_list)


def solution(mesh):
    axes = ("gx", "gy", "gz")
    sizes = tuple(mesh.shape[name] for name in axes)
    return jax.shard_map(
        functools.partial(per_device, axes, sizes),
        mesh=mesh,
        in_specs=(
            P(None, "gx", "gy", "gz", None),
            P(None, "gx", "gy", "gz", None),
            P("gx", "gy", "gz", None),
            P("gx", "gy", "gz", None),
            P("gx", "gy", "gz", None),
            P("gx", "gy", "gz", None),
        ),
        out_specs=(P(None, "gx", "gy", "gz", None), P("gx", "gy", "gz", None)),
        check_vma=False,
    )
```

```python
import functools

import jax
import jax.numpy as jnp
from jax import lax
from jax.experimental import pallas as pl
from jax.experimental.pallas import tpu as pltpu
from jax.sharding import PartitionSpec as P

ORDER = 4
LANES = 128
SUBS = 8
F32, BF16, I32 = jnp.float32, jnp.bfloat16, jnp.int32
MESH = pl.DeviceIdType.MESH
SYM = ((0, 0), (0, 1), (0, 2), (1, 1), (1, 2), (2, 2))


def dot_nt(left, right):
    return lax.dot_general(left, right, (((1,), (1,)), ((), ())), preferred_element_type=F32)


def dot_nn(left, right):
    return lax.dot_general(left, right, (((1,), (0,)), ((), ())), preferred_element_type=F32)


def wide(row, count=SUBS):
    return jnp.broadcast_to(row, (count, row.shape[1]))


def lanes_at(rows, index):
    return jnp.take_along_axis(rows, index, axis=1, mode="promise_in_bounds")


def subs_at(rows, index):
    return jnp.take_along_axis(rows, index, axis=0, mode="promise_in_bounds")


def split(value, count=2):
    parts = []
    for _ in range(count - 1):
        high = value.astype(BF16).astype(F32)
        parts.append(high)
        value = value - high
    return parts + [value]


def flips(n):
    return n >= 4 and n % 2 == 0


def routes(sizes):
    plane = [(a, c) for a in range(3) for c in range(3)]
    classes = [(a, b, c) for b in (0, 2, 1) for a, c in plane[:SUBS]]
    classes += [plane[SUBS][:1] + (b,) + plane[SUBS][1:] for b in (0, 2, 1)]
    direct, forth, back = [], [], []
    for cls in classes:
        direct.append(tuple((1 - c) for c in cls))
        forth.append(tuple((0, 1, -2)[c] if flips(n) else c - 1 for c, n in zip(cls, sizes)))
        back.append(tuple((0, 1, 2)[c] if flips(n) else 1 - c for c, n in zip(cls, sizes)))
    return classes, direct, forth, back


def kernel(
    axes, sizes, send_count,
    old_hbm, move_hbm, mass_hbm, head_hbm, tail_hbm, send_hbm,
    pos_ref, mult_ref,
    old_ref, move_ref, mass_ref, head_ref, tail_ref, send_ref, load_sem,
    table, hot_head, hot_tail, hot_root, mask_tail, mask_root, stage,
    out0, in0, out1, in1, out2, in2, out3, in3, out4, in4,
    send_sem, recv_sem,
):
    atoms, bonds = old_ref.shape[-1], head_ref.shape[-1]
    atom_rows, bond_rows = atoms // LANES, bonds // LANES
    slot_rows = bond_rows + -(-(atoms - bonds) // LANES)
    width = send_count
    bits = width.bit_length() - 1
    classes, direct, forth, back = routes(sizes)
    centre = classes.index((1, 1, 1))
    hub_row = classes.index(tuple(0 if flips(n) else 1 for n in sizes))
    tiles = -(-len(classes) // SUBS)
    here = [lax.axis_index(name) for name in axes]
    turn = [1 - 2 * lax.rem(i, 2) if flips(n) else 1 for i, n in zip(here, sizes)]

    twin = sizes[1] == 2

    def nowhere(offset):
        return all(o % n == 0 for o, n in zip(offset, sizes))

    def target(offset):
        return tuple(
            lax.rem(i + o * s + 2 * n, n) for i, o, s, n in zip(here, offset, turn, sizes)
        )

    greet = []
    for group in (direct, forth, back):
        for offset in group:
            key = tuple(o % n for o, n in zip(offset, sizes))
            if any(key) and key not in [k for k, _ in greet]:
                greet.append((key, offset))
    loads = [
        pltpu.make_async_copy(source, dest, load_sem.at[i])
        for i, (source, dest) in enumerate((
            (send_hbm, send_ref), (old_hbm, old_ref), (move_hbm, move_ref), (mass_hbm, mass_ref),
            (head_hbm, head_ref), (tail_hbm, tail_ref),
        ))
    ]
    for load in loads:
        load.start()
    barrier = pltpu.get_barrier_semaphore()
    for _, offset in greet:
        pl.semaphore_signal(barrier, inc=1, device_id=target(offset), device_id_type=MESH)

    sub = lax.broadcasted_iota(I32, (SUBS, LANES), 0)
    lane = lax.broadcasted_iota(I32, (SUBS, LANES), 1)
    group = lax.shift_right_logical(lane, bits)
    entry = lane & (width - 1)
    swap = (group - sub) & (SUBS - 1)
    unskew = (lane + width * sub) & (LANES - 1)

    def transpose8(x):
        x = pltpu.roll(x, 0, 1, stride=width, stride_axis=0)
        return lanes_at(subs_at(x, swap), unskew)

    for load in loads:
        load.wait()

    old = [old_ref[k, 0, 0].reshape(atom_rows, LANES) for k in range(3)]
    pos0 = [old[k] + move_ref[k, 0, 0].reshape(atom_rows, LANES) for k in range(3)]
    mass = mass_ref[0, 0].reshape(atom_rows, LANES)
    values = old + pos0 + [mass, jnp.zeros((atom_rows, LANES), F32)]
    for g, value in enumerate(values):
        for q in range(atom_rows):
            table[SUBS * q + g : SUBS * q + g + 1, :] = value[q : q + 1]
    send_row = jnp.concatenate(
        [send_ref[0, 0], jnp.zeros((1, LANES - send_count), I32)], axis=1
    )
    send_rep = lanes_at(wide(send_row), entry)
    send_tile, send_lane = lax.shift_right_logical(send_rep, 7), send_rep & (LANES - 1)
    found = jnp.zeros((SUBS, LANES), F32)
    for q in range(atom_rows):
        found = jnp.where(
            send_tile == q, lanes_at(table[SUBS * q : SUBS * q + SUBS, :], send_lane), found
        )
    found = jnp.sum(jnp.where(group == sub, found, 0.0), axis=0, keepdims=True)
    out0[0] = wide(found)
    for land in (in1, in3):
        for part in range(land.shape[0]):
            land[part, centre : centre + 1, :] = jnp.zeros((1, LANES), F32)
            land[part, len(classes) :, :] = jnp.zeros((SUBS * tiles - len(classes), LANES), F32)
            if twin and land is in3:
                land[part, 3 * SUBS + 1 : 3 * SUBS + 2, :] = jnp.zeros((1, LANES), F32)
    head = head_ref[0, 0].reshape(bond_rows, LANES)
    tail = tail_ref[0, 0].reshape(bond_rows, LANES)
    head_tile, head_lane = lax.shift_right_logical(head, 7), head & (LANES - 1)
    tail_tile, tail_lane = lax.shift_right_logical(tail, 7), tail & (LANES - 1)
    is_far = tail >= atoms
    slot = jnp.maximum(tail - atoms, 0)
    block = lax.shift_right_logical(slot, bits)
    one = lambda test: jnp.where(test, 1, 0)
    bx = one(block >= 9) + one(block >= 18)
    rest = block - 9 * bx
    by = one(rest >= 3) + one(rest >= 6)
    bz = rest - 3 * by
    place = [
        1 - s * (b - 1) if flips(n) else b
        for b, s, n in zip((bx, by, bz), turn, sizes)
    ]
    across_plane = place[0] * 3 + place[2]
    level = jnp.where(place[1] == 0, 0, 3 - place[1])
    slot_row = jnp.where(across_plane < SUBS, SUBS * level + across_plane, 3 * SUBS + level)
    slot = slot_row * width + (slot & (width - 1))

    def gather(rows, tile, index, start=0.0, count=None):
        shape = index.shape
        total = jnp.full(shape, start, rows.dtype)
        for q in range(count or rows.shape[0]):
            total = jnp.where(tile == q, lanes_at(wide(rows[q : q + 1], shape[0]), index), total)
        return total

    deep = lax.broadcasted_iota(I32, (LANES, LANES), 0)
    across = lax.broadcasted_iota(I32, (LANES, LANES), 1)
    row16 = lax.broadcasted_iota(I32, (2 * SUBS, LANES), 0)
    parts = []
    for s in range(bond_rows):
        hot_head[:, s * LANES : (s + 1) * LANES] = jnp.where(
            deep == wide(head_lane[s : s + 1], LANES), 1.0, 0.0
        ).astype(BF16)
        number = lane[0:1] + (s * LANES + 1)
        high = (number - (number & 7)).astype(F32)
        low = (number & 7).astype(F32)
        match = row16 == wide(head_tile[s : s + 1], 2 * SUBS)
        parts.append(jnp.concatenate(
            [jnp.where(match, wide(high, 16), 0.0), jnp.where(match, wide(low, 16), 0.0)], axis=0
        ).astype(BF16))
    owner_of = dot_nt(jnp.concatenate(parts, axis=1), hot_head[...])
    owner_of = owner_of[:16] + owner_of[16:]
    free = jnp.where(owner_of == 0.0, 1.0, 0.0).astype(BF16)
    before = dot_nn(free, jnp.where(deep < across, 1.0, 0.0).astype(BF16))
    totals = dot_nn(free, jnp.ones((LANES, LANES), BF16))
    for q in range(atom_rows - 1):
        before = before + jnp.where(row16 > q, wide(totals[q : q + 1], 16), 0.0)
    place_of = jnp.where(owner_of > 0.0, owner_of - 1.0, before + float(bonds)).astype(I32)
    spot = gather(place_of, tail_tile, tail_lane, 0, atom_rows)
    spot = jnp.where(is_far, -1, spot)
    spot_tile, spot_lane = lax.shift_right_arithmetic(spot, 7), spot & (LANES - 1)

    label = jnp.where(is_far, slot, -1)
    for _ in range(ORDER + 1):
        label = jnp.where(is_far, slot, gather(label, spot_tile, spot_lane, -1))
    label_tile, label_lane = lax.shift_right_arithmetic(label, 7), label & (LANES - 1)

    def columns(index, dest):
        col = index.astype(F32).T
        line = lane[0:1].astype(F32)
        for s in range(bond_rows):
            dest[s * LANES : (s + 1) * LANES, :] = jnp.where(
                col[:, s : s + 1] == line, 1.0, 0.0
            ).astype(BF16)

    columns(spot_lane, hot_tail)
    columns(label_lane, hot_root)
    for s in range(bond_rows):
        mask_tail[16 * s : 16 * s + 16, :] = jnp.where(
            row16 == wide(spot_tile[s : s + 1], 16), 1.0, 0.0
        ).astype(BF16)
        for q in range(tiles):
            base = 16 * (s * tiles + q)
            mask_root[base : base + 16, :] = jnp.where(
                wide(label_tile[s : s + 1], 16) == q, 1.0, 0.0
            ).astype(BF16)

    old_pos = old + pos0 + [mass]
    at_head = [gather(v, head_tile, head_lane) for v in old_pos]
    at_tail = [gather(v, tail_tile, tail_lane) for v in old_pos]

    def scatter(rows):
        halves = [half for row in rows for half in split(row)]
        parts = []
        for s in range(bond_rows):
            mask = mask_tail[16 * s : 16 * s + 16, :]
            parts.append(jnp.concatenate(
                [wide(half[s : s + 1], 16).astype(BF16) * mask for half in halves], axis=0
            ))
        out = dot_nn(jnp.concatenate(parts, axis=1), hot_tail[...])
        return [out[32 * i : 32 * i + 16] + out[32 * i + 16 : 32 * i + 32] for i in range(len(rows))]

    def spread(bent, rows):
        pulls = [bent[d] * row for row in rows for d in range(3)]
        sums = scatter(pulls)
        return [
            jnp.concatenate([p - t[:bond_rows], -t[bond_rows:slot_rows]], axis=0)
            for p, t in zip(pulls, sums)
        ], sums

    def meet(moves):
        return [
            mass_head * m[:bond_rows] - near_mass * gather(m, spot_tile, spot_lane) for m in moves
        ]

    def bend(bent, vector):
        return bent[0] * vector[0] + bent[1] * vector[1] + bent[2] * vector[2]

    def to_slots(rows, pieces=2):
        count = -(-len(rows) // SUBS)
        half = SUBS * count
        pad = pieces * count % 2
        for v in range(half):
            stage[SUBS * v : SUBS * v + SUBS, :] = (
                rows[v] if v < len(rows) else jnp.zeros((SUBS, LANES), F32)
            )
        parts = []
        for s in range(bond_rows):
            value = jnp.concatenate(
                [stage[pl.ds(SUBS * SUBS * c + s, SUBS, stride=SUBS), :] for c in range(count)], axis=0
            )
            layers = split(value, pieces) + [jnp.zeros((SUBS, LANES), F32)] * pad
            both = jnp.concatenate(layers, axis=0).astype(BF16)
            size = both.shape[0]
            chunks = []
            for q in range(tiles):
                base = 16 * (s * tiles + q)
                mask = mask_root[base : base + 16, :]
                chunks.append(both * jnp.concatenate([mask] * (size // 16), axis=0))
            parts.append(jnp.concatenate(chunks, axis=0))
        out = dot_nn(jnp.concatenate(parts, axis=1), hot_root[...])
        result = []
        for q in range(tiles):
            found = []
            for c in range(count):
                base = size * q + SUBS * c
                found.append(sum(
                    [out[base + half * p : base + half * p + SUBS] for p in range(1, pieces)],
                    out[base : base + SUBS],
                ))
            result.append(found)
        return result

    def to_bonds(slots, row):
        total = jnp.zeros((bond_rows, LANES), F32)
        for q in range(tiles):
            total = jnp.where(
                label_tile == q, lanes_at(wide(slots[q][row : row + 1], bond_rows), label_lane), total
            )
        return total

    flags = jnp.where(is_far, 1.0, 0.0)
    order = sorted(range(len(classes)), key=lambda r: -(classes[r][0] + classes[r][2]))

    def copies(step, source, landing, offsets, each, whole, merge=True, only=None):
        started = {}
        for row in only or order:
            if row == centre and not whole or merge and twin and classes[row][1] == 2:
                continue
            line = row if each else 0
            if nowhere(offsets[row]):
                landing[:, row : row + 1, :] = source[:, line : line + 1, :]
                continue
            copy = pltpu.make_async_remote_copy(
                source.at[:, line], landing.at[:, row],
                send_sem.at[step, row], recv_sem.at[step, row],
                device_id=target(offsets[row]), device_id_type=MESH,
            )
            copy.start()
            started[row] = copy
        return started

    def post(out, part, value):
        pieces = [value[SUBS * q : SUBS * q + SUBS] for q in range(tiles)]
        if twin:
            pieces[0] = pieces[0] + pieces[1]
            pieces[3] = pieces[3] + jnp.where(sub == 0, wide(pieces[3][1:2]), 0.0)
        for q in range(tiles):
            if not (twin and q == 1):
                out[part, SUBS * q : SUBS * q + SUBS, :] = pieces[q]

    def landed(land, part):
        parts = [land[part, SUBS * q : SUBS * q + SUBS, :] for q in range(tiles)]
        if twin:
            parts[1] = parts[0]
            parts[3] = jnp.where(sub == 1, wide(parts[3][0:1]), parts[3])
        return parts

    pending = []

    def arrive(started):
        for copy in started:
            copy.wait_recv()
            pending.append(copy)


    mass_head = at_head[6]

    def geometry(head_data, tail_data):
        olds = [head_data[d] - tail_data[d] for d in range(3)]
        news = [head_data[3 + d] - tail_data[3 + d] for d in range(3)]
        size = jnp.maximum(jnp.sqrt(olds[0] * olds[0] + olds[1] * olds[1] + olds[2] * olds[2]), 0.5)
        direction = [b / size for b in olds]
        scale = 1.0 / jnp.sqrt(head_data[6] + tail_data[6])
        right = scale * (
            direction[0] * news[0] + direction[1] * news[1] + direction[2] * news[2] - size
        )
        return news, size, scale, [scale * d for d in direction], right

    _, _, _, bent, right = geometry(at_head, at_tail)
    bent = [jnp.where(is_far, 0.0, b) for b in bent]
    near_mass = jnp.where(is_far, 0.0, at_tail[6])
    kids = gather(flags, spot_tile, spot_lane) * near_mass
    series = [jnp.where(is_far, 0.0, right)] + [kids * b for b in bent]
    couplings = [series]
    for k in range(ORDER - 2):
        moves, _ = spread(bent, series)
        meets = meet(moves)
        series = [v - bend(bent, meets[3 * i : 3 * i + 3]) for i, v in enumerate(series)]
        couplings.append(series)
        series = series[:1]
    once = couplings[1][1:]
    zero = couplings[0][1:]
    drive = [[g * couplings[0][0] for g in zero]] + [
        [g * c[0] for g in once] for c in couplings
    ]
    square_of = [
        [left[a] * other[b] for a, b in SYM]
        for left, other in ((zero, zero), (once, zero), (once, once))
    ]

    spread_lane = width * sub + entry

    def to_rows(packed, row):
        return jnp.concatenate(
            [lanes_at(wide(packed[q][row : row + 1]), spread_lane) for q in range(tiles)], axis=0
        )

    drives = to_slots([v for group in drive + square_of for v in group])
    places = to_slots([v * flags for v in at_head], 3)
    for q in range(tiles):
        for c, part in enumerate(places[q] + drives[q]):
            out1[c, SUBS * q : SUBS * q + SUBS, :] = transpose8(part)
    pl.semaphore_wait(barrier, len(greet))
    hub_first = copies(0, out0, in0, direct, False, False, only=(hub_row,))
    second = copies(1, out1, in1, forth, True, False, merge=False)
    others = tuple(row for row in order if row != hub_row)
    first = copies(0, out0, in0, direct, False, False, only=others)

    entry_rows = jnp.concatenate([entry] * tiles, axis=0)
    group_rows = jnp.concatenate([group] * tiles, axis=0)

    def packed(values):
        total = jnp.zeros((SUBS * tiles, LANES), F32)
        for g, value in enumerate(values):
            total = jnp.where(group_rows == g, value, total)
        return total

    def post_terms(values, out):
        steps = [normal[d] * values[k] for k in range(ORDER + 1) for d in range(3)]
        post(out, 0, packed(steps[:SUBS]))
        post(out, 1, packed(steps[SUBS:]))

    arrive(hub_first.values())
    arrive(second.values())
    heavy = in0[0, hub_row : hub_row + 1, :] if hub_row != centre else out0[0, 0:1, :]
    sent_data = [lanes_at(wide(heavy), entry + width * g) for g in range(7)]
    mass_send = sent_data[6]
    arrived = [
        lanes_at(in1[v // SUBS], entry_rows + width * (v % SUBS))
        for v in range(SUBS + 3 * ORDER + 6 * (ORDER - 1))
    ]
    head_rows, flat = arrived[:7], arrived[SUBS:]
    drive = [flat[3 * k : 3 * k + 3] for k in range(ORDER)]
    square_of = [flat[3 * ORDER + 6 * k : 3 * ORDER + 6 * k + 6] for k in range(ORDER - 1)]
    _, _, _, normal, start = geometry(
        head_rows, [jnp.concatenate([v] * tiles, axis=0) for v in sent_data]
    )
    normal = [jnp.where(head_rows[6] > 0.0, b, 0.0) for b in normal]
    pairs = [normal[a] * normal[b] for a, b in SYM]
    keep = 1.0 - head_rows[6] * (pairs[0] + pairs[3] + pairs[5])
    pushes = [
        q[0] * pairs[0] + q[3] * pairs[3] + q[5] * pairs[5]
        + 2.0 * (q[1] * pairs[1] + q[2] * pairs[2] + q[4] * pairs[4])
        for q in square_of
    ]
    chain, reply = [start], [None, keep]
    for k in range(1, ORDER + 1):
        value = keep * chain[-1] + (
            normal[0] * drive[k - 1][0] + normal[1] * drive[k - 1][1] + normal[2] * drive[k - 1][2]
        )
        for i in range(k - 1):
            value = value + pushes[k - 2 - i] * chain[i]
        chain.append(value)
    for k in range(2, ORDER):
        value = keep * reply[-1] + pushes[k - 2]
        for i in range(1, k - 1):
            value = value + pushes[k - 2 - i] * reply[i]
        reply.append(value)

    def summed(value):
        total = value[:SUBS]
        for q in range(1, tiles):
            total = total + value[SUBS * q : SUBS * q + SUBS]
        for shift in (4, 2, 1):
            total = total + pltpu.roll(total, shift, 0)
        return total

    got = [summed(normal[d] * chain[k]) for k in range(ORDER + 1) for d in range(3)]
    matrix = [
        {
            ab: -mass_send * summed(p if reply[g] is None else reply[g] * p)
            for ab, p in zip(SYM, pairs)
        }
        for g in range(ORDER)
    ]
    def collect(land):
        found = []
        for part in range(land.shape[0]):
            total = land[part, 0:SUBS, :]
            for q in range(1, tiles):
                if not (twin and q == 1):
                    total = total + land[part, SUBS * q : SUBS * q + SUBS, :]
            for shift in (4, 2, 1):
                total = total + pltpu.roll(total, shift, 0)
            for g in range(SUBS):
                found.append(lanes_at(total, entry + width * g))
        return found

    def owner(got, out):
        moved = []
        for k in range(ORDER + 1):
            total = [-mass_send * got[3 * k + d] for d in range(3)]
            for i in range(k):
                push = matrix[k - 1 - i]
                for d in range(3):
                    for e in range(3):
                        total[d] = total[d] + push[(min(d, e), max(d, e))] * moved[i][e]
            moved.append(total)
        for c in range(2):
            message = jnp.zeros((SUBS, LANES), F32)
            for g in range(SUBS):
                v = SUBS * c + g
                if v < 3 * ORDER:
                    value = moved[v % ORDER][v // ORDER]
                elif v < 3 * ORDER + 3:
                    value = sum([m[v - 3 * ORDER] for m in moved[1:]], moved[0][v - 3 * ORDER])
                else:
                    continue
                message = jnp.where(group == g, value, message)
            out[c] = message

    owner(got, out2)
    third = copies(2, out2, in2, back, False, True)

    arrive(first.values())
    far = [transpose8(piece) for piece in landed(in0, 0)]
    at_tail = [jnp.where(is_far, to_bonds(far, g), v) for g, v in enumerate(at_tail)]
    bond_new, length, scale, bent, right1 = geometry(at_head, at_tail)
    normal = [part[0] for part in to_slots([b * flags for b in bent])]
    upper = jnp.where(sub < 4, 0, 1)
    normal_a = [subs_at(n, upper) for n in normal]
    normal_b = [wide(n[2:3]) for n in normal]
    normal = [to_rows(normal, d) for d in range(3)]

    terms, fars = [right1], [flags]
    term_moves, term_meets, far_moves, far_meets = [], [], [], []

    def advance():
        moves, _ = spread(bent, [terms[-1], fars[-1]])
        meets = meet(moves)
        term_moves.append(moves[:3])
        far_moves.append(moves[3:])
        term_meets.append(meets[:3])
        far_meets.append(meets[3:])
        terms.append(terms[-1] - bend(bent, meets[:3]))
        fars.append(fars[-1] - bend(bent, meets[3:]))

    for _ in range(ORDER):
        advance()
    last_moves, _ = spread(bent, [terms[ORDER]])
    last_meets = meet(last_moves)
    base1 = sum(terms[1:], terms[0])

    weights, weight_moves, weight_meets = [], [], []
    for k in range(ORDER):
        if k == 0:
            weights.append(fars[0])
            weight_moves.append(far_moves[0])
            weight_meets.append(far_meets[0])
        else:
            weights.append(weights[-1] + fars[k])
            weight_moves.append([a + b for a, b in zip(weight_moves[-1], far_moves[k])])
            weight_meets.append([a + b for a, b in zip(weight_meets[-1], far_meets[k])])
    base_moves = [sum([m[d] for m in term_moves], last_moves[d]) for d in range(3)]
    base_meets = [sum([m[d] for m in term_meets], last_meets[d]) for d in range(3)]

    def answers(land):
        low = [transpose8(piece) for piece in landed(land, 0)]
        high = [transpose8(piece) for piece in landed(land, 1)]
        replies = []
        for q in range(tiles):
            product = low[q] * normal_a[q]
            replies.append(product + pltpu.roll(product, 4, 0) + high[q] * normal_b[q])
        return replies, high

    def through(weights, injected):
        total = weights[0] * injected[ORDER - 1]
        for k in range(1, ORDER):
            total = total + weights[k] * injected[ORDER - 1 - k]
        return total

    arrive(third.values())
    replies1, high = answers(in2)
    injected1 = [to_bonds(replies1, k) for k in range(ORDER)]
    tail_moves = [to_bonds(high, 4 + d) for d in range(3)]
    sol1 = base1 + through(weights, injected1)
    stretch = [
        bond_new[d]
        - (base_meets[d] + through([w[d] for w in weight_meets], injected1) - flags * tail_moves[d])
        for d in range(3)
    ]
    current = stretch[0] * stretch[0] + stretch[1] * stretch[1] + stretch[2] * stretch[2]
    square = length * length
    goal = jnp.sqrt(jnp.maximum(2.0 * square - current, 0.5 * square))
    right2 = scale * (length - goal)
    slots3 = to_slots([fars[k] * right2 for k in range(ORDER + 1)])
    slots3 = [part[0] for part in slots3]
    post_terms([to_rows(slots3, k) for k in range(ORDER + 1)], out3)
    fourth = copies(3, out3, in3, forth, True, False)

    term, both = right2, sol1 + right2
    for k in range(ORDER + 1):
        moves, _ = spread(bent, [term])
        base_moves = [a + b for a, b in zip(base_moves, moves)]
        if k < ORDER:
            term = term - bend(bent, meet(moves))
            both = both + term
        if k == 1:
            arrive(fourth.values())
            owner(collect(in3), out4)
            fifth = copies(4, out4, in4, back, False, True)

    place_tile = lax.shift_right_logical(place_of[:atom_rows], 7)
    place_lane = place_of[:atom_rows] & (LANES - 1)
    number = lax.broadcasted_iota(I32, (atom_rows, LANES), 0) * LANES + lax.broadcasted_iota(
        I32, (atom_rows, LANES), 1
    )
    entry_of = jnp.full((atom_rows, LANES), -1, I32)
    for e in range(send_count):
        entry_of = jnp.where(number == wide(send_rep[0:1, e : e + 1] + jnp.zeros((1, LANES), I32), atom_rows), e, entry_of)
    sent = entry_of >= 0
    entry_of = jnp.maximum(entry_of, 0)

    atom_label = jnp.where(
        place_tile < bond_rows, gather(label, place_tile, place_lane, -1, bond_rows), -1
    )
    atom_tile, atom_lane = lax.shift_right_arithmetic(atom_label, 7), atom_label & (LANES - 1)
    at_atoms = [pos0[d] - mass * gather(base_moves[d], place_tile, place_lane) for d in range(3)]
    weight_moves = [
        [mass * gather(w[d][:bond_rows], place_tile, place_lane) for d in range(3)]
        for w in weight_moves
    ]
    early = len(pending)
    for copy in pending:
        copy.wait_send()

    arrive(fifth.values())
    replies2, _ = answers(in4)
    both = both + through(weights, [to_bonds(replies2, k) for k in range(ORDER)])
    mult_ref[0, 0] = both.reshape(1, bonds)
    replies = [a + b for a, b in zip(replies1, replies2)]
    injected = []
    for k in range(ORDER):
        total = jnp.zeros((atom_rows, LANES), F32)
        for q in range(tiles):
            total = jnp.where(
                atom_tile == q, lanes_at(wide(replies[q][k : k + 1], atom_rows), atom_lane), total
            )
        injected.append(total)
    own = wide(in2[1, centre : centre + 1, :] + in4[1, centre : centre + 1, :], atom_rows)
    for d in range(3):
        result = at_atoms[d] - through([w[d] for w in weight_moves], injected)
        result = result - jnp.where(sent, lanes_at(own, entry_of + width * (4 + d)), 0.0)
        pos_ref[d, 0, 0] = result.reshape(1, atoms)
    for copy in pending[early:]:
        copy.wait_send()


def per_device(axes, sizes, old_pos, displacement, inv_mass, bond_head, bond_tail, send_list):
    atoms, bonds, send_count = old_pos.shape[-1], bond_head.shape[-1], send_list.shape[-1]
    rows = 4 * SUBS
    vmem = lambda *shape: pltpu.VMEM(shape + (LANES,), F32)
    half = lambda *shape: pltpu.VMEM(shape, BF16)
    bond_rows = bonds // LANES
    return pl.pallas_call(
        functools.partial(kernel, axes, sizes, send_count),
        out_shape=(
            pltpu.VMEM(old_pos.shape, F32),
            pltpu.VMEM(bond_head.shape, F32),
        ),
        in_specs=[pl.BlockSpec(memory_space=pltpu.HBM)] * 6,
        out_specs=(pl.BlockSpec(memory_space=pltpu.VMEM), pl.BlockSpec(memory_space=pltpu.VMEM)),
        scratch_shapes=[
            pltpu.VMEM(old_pos.shape, F32), pltpu.VMEM(displacement.shape, F32),
            pltpu.VMEM(inv_mass.shape, F32), pltpu.VMEM(bond_head.shape, I32),
            pltpu.VMEM(bond_tail.shape, I32), pltpu.VMEM(send_list.shape, I32),
            pltpu.SemaphoreType.DMA((6,)),
            vmem(atoms // LANES * SUBS),
            half(LANES, bonds), half(bonds, LANES), half(bonds, LANES),
            half(16 * bond_rows, LANES), half(16 * bond_rows * 4, LANES),
            vmem(4 * SUBS * SUBS),
            vmem(1, SUBS), vmem(1, rows),
            vmem(5, rows), vmem(5, rows),
            vmem(2, SUBS), vmem(2, rows),
            vmem(2, rows), vmem(2, rows),
            vmem(2, SUBS), vmem(2, rows),
            pltpu.SemaphoreType.DMA((5, 27)),
            pltpu.SemaphoreType.DMA((5, 27)),
        ],
        compiler_params=pltpu.CompilerParams(
            collective_id=0, has_side_effects=True, vmem_limit_bytes=56 * 1024 * 1024
        ),
    )(old_pos, displacement, inv_mass, bond_head, bond_tail, send_list)


def solution(mesh):
    axes = ("gx", "gy", "gz")
    sizes = tuple(mesh.shape[name] for name in axes)
    return jax.shard_map(
        functools.partial(per_device, axes, sizes),
        mesh=mesh,
        in_specs=(
            P(None, "gx", "gy", "gz", None),
            P(None, "gx", "gy", "gz", None),
            P("gx", "gy", "gz", None),
            P("gx", "gy", "gz", None),
            P("gx", "gy", "gz", None),
            P("gx", "gy", "gz", None),
        ),
        out_specs=(P(None, "gx", "gy", "gz", None), P("gx", "gy", "gz", None)),
        check_vma=False,
    )
```

```python
import functools

import jax
import jax.numpy as jnp
from jax import lax
from jax.experimental import pallas as pl
from jax.experimental.pallas import tpu as pltpu
from jax.sharding import PartitionSpec as P

ORDER = 4
LANES = 128
SUBS = 8
F32, BF16, I32 = jnp.float32, jnp.bfloat16, jnp.int32
MESH = pl.DeviceIdType.MESH
SYM = ((0, 0), (0, 1), (0, 2), (1, 1), (1, 2), (2, 2))


def dot_nt(left, right):
    return lax.dot_general(left, right, (((1,), (1,)), ((), ())), preferred_element_type=F32)


def dot_nn(left, right):
    return lax.dot_general(left, right, (((1,), (0,)), ((), ())), preferred_element_type=F32)


def wide(row, count=SUBS):
    return jnp.broadcast_to(row, (count, row.shape[1]))


def lanes_at(rows, index):
    return jnp.take_along_axis(rows, index, axis=1, mode="promise_in_bounds")


def subs_at(rows, index):
    return jnp.take_along_axis(rows, index, axis=0, mode="promise_in_bounds")


def split(value, count=2):
    parts = []
    for _ in range(count - 1):
        high = value.astype(BF16).astype(F32)
        parts.append(high)
        value = value - high
    return parts + [value]


def flips(n):
    return n >= 4 and n % 2 == 0


def routes(sizes):
    plane = [(a, c) for a in range(3) for c in range(3)]
    classes = [(a, b, c) for b in (0, 2, 1) for a, c in plane[:SUBS]]
    classes += [plane[SUBS][:1] + (b,) + plane[SUBS][1:] for b in (0, 2, 1)]
    direct, forth, back = [], [], []
    for cls in classes:
        direct.append(tuple((1 - c) for c in cls))
        forth.append(tuple((0, 1, -2)[c] if flips(n) else c - 1 for c, n in zip(cls, sizes)))
        back.append(tuple((0, 1, 2)[c] if flips(n) else 1 - c for c, n in zip(cls, sizes)))
    return classes, direct, forth, back


def kernel(
    axes, sizes, send_count,
    old_hbm, move_hbm, mass_hbm, head_hbm, tail_hbm, send_hbm,
    pos_ref, mult_ref,
    old_ref, move_ref, mass_ref, head_ref, tail_ref, send_ref, load_sem,
    table, hot_head, hot_tail, hot_root, mask_tail, mask_root, stage,
    out0, in0, out1, in1, out2, in2, out3, in3, out4, in4,
    spare, send_sem, recv_sem,
):
    atoms, bonds = old_ref.shape[-1], head_ref.shape[-1]
    atom_rows, bond_rows = atoms // LANES, bonds // LANES
    slot_rows = bond_rows + -(-(atoms - bonds) // LANES)
    width = send_count
    bits = width.bit_length() - 1
    classes, direct, forth, back = routes(sizes)
    centre = classes.index((1, 1, 1))
    hub_row = classes.index(tuple(0 if flips(n) else 1 for n in sizes))
    tiles = -(-len(classes) // SUBS)
    here = [lax.axis_index(name) for name in axes]
    turn = [1 - 2 * lax.rem(i, 2) if flips(n) else 1 for i, n in zip(here, sizes)]

    twin = sizes[1] == 2

    def nowhere(offset):
        return all(o % n == 0 for o, n in zip(offset, sizes))

    def target(offset):
        return tuple(
            lax.rem(i + o * s + 2 * n, n) for i, o, s, n in zip(here, offset, turn, sizes)
        )

    greet = []
    for group in (direct, forth, back):
        for offset in group:
            key = tuple(o % n for o, n in zip(offset, sizes))
            if any(key) and key not in [k for k, _ in greet]:
                greet.append((key, offset))
    loads = [
        pltpu.make_async_copy(source, dest, load_sem.at[i])
        for i, (source, dest) in enumerate((
            (send_hbm, send_ref), (old_hbm, old_ref), (move_hbm, move_ref), (mass_hbm, mass_ref),
            (head_hbm, head_ref), (tail_hbm, tail_ref),
        ))
    ]
    for load in loads:
        load.start()
    barrier = pltpu.get_barrier_semaphore()
    for _, offset in greet:
        pl.semaphore_signal(barrier, inc=1, device_id=target(offset), device_id_type=MESH)

    sub = lax.broadcasted_iota(I32, (SUBS, LANES), 0)
    lane = lax.broadcasted_iota(I32, (SUBS, LANES), 1)
    group = lax.shift_right_logical(lane, bits)
    entry = lane & (width - 1)
    swap = (group - sub) & (SUBS - 1)
    unskew = (lane + width * sub) & (LANES - 1)

    def transpose8(x):
        x = pltpu.roll(x, 0, 1, stride=width, stride_axis=0)
        return lanes_at(subs_at(x, swap), unskew)

    for load in loads:
        load.wait()

    old = [old_ref[k, 0, 0].reshape(atom_rows, LANES) for k in range(3)]
    pos0 = [old[k] + move_ref[k, 0, 0].reshape(atom_rows, LANES) for k in range(3)]
    mass = mass_ref[0, 0].reshape(atom_rows, LANES)
    values = old + pos0 + [mass, jnp.zeros((atom_rows, LANES), F32)]
    for g, value in enumerate(values):
        for q in range(atom_rows):
            table[SUBS * q + g : SUBS * q + g + 1, :] = value[q : q + 1]
    send_row = jnp.concatenate(
        [send_ref[0, 0], jnp.zeros((1, LANES - send_count), I32)], axis=1
    )
    send_rep = lanes_at(wide(send_row), entry)
    send_tile, send_lane = lax.shift_right_logical(send_rep, 7), send_rep & (LANES - 1)
    found = jnp.zeros((SUBS, LANES), F32)
    for q in range(atom_rows):
        found = jnp.where(
            send_tile == q, lanes_at(table[SUBS * q : SUBS * q + SUBS, :], send_lane), found
        )
    found = jnp.sum(jnp.where(group == sub, found, 0.0), axis=0, keepdims=True)
    out0[0] = wide(found)
    for land in (in1, in3):
        for part in range(land.shape[0]):
            land[part, centre : centre + 1, :] = jnp.zeros((1, LANES), F32)
            land[part, len(classes) :, :] = jnp.zeros((SUBS * tiles - len(classes), LANES), F32)
            if twin and land is in3:
                land[part, 3 * SUBS + 1 : 3 * SUBS + 2, :] = jnp.zeros((1, LANES), F32)
    head = head_ref[0, 0].reshape(bond_rows, LANES)
    tail = tail_ref[0, 0].reshape(bond_rows, LANES)
    head_tile, head_lane = lax.shift_right_logical(head, 7), head & (LANES - 1)
    tail_tile, tail_lane = lax.shift_right_logical(tail, 7), tail & (LANES - 1)
    is_far = tail >= atoms
    slot = jnp.maximum(tail - atoms, 0)
    block = lax.shift_right_logical(slot, bits)
    one = lambda test: jnp.where(test, 1, 0)
    bx = one(block >= 9) + one(block >= 18)
    rest = block - 9 * bx
    by = one(rest >= 3) + one(rest >= 6)
    bz = rest - 3 * by
    place = [
        1 - s * (b - 1) if flips(n) else b
        for b, s, n in zip((bx, by, bz), turn, sizes)
    ]
    across_plane = place[0] * 3 + place[2]
    level = jnp.where(place[1] == 0, 0, 3 - place[1])
    slot_row = jnp.where(across_plane < SUBS, SUBS * level + across_plane, 3 * SUBS + level)
    slot = slot_row * width + (slot & (width - 1))

    def gather(rows, tile, index, start=0.0, count=None):
        shape = index.shape
        total = jnp.full(shape, start, rows.dtype)
        for q in range(count or rows.shape[0]):
            total = jnp.where(tile == q, lanes_at(wide(rows[q : q + 1], shape[0]), index), total)
        return total

    deep = lax.broadcasted_iota(I32, (LANES, LANES), 0)
    across = lax.broadcasted_iota(I32, (LANES, LANES), 1)
    row16 = lax.broadcasted_iota(I32, (2 * SUBS, LANES), 0)
    parts = []
    for s in range(bond_rows):
        hot_head[:, s * LANES : (s + 1) * LANES] = jnp.where(
            deep == wide(head_lane[s : s + 1], LANES), 1.0, 0.0
        ).astype(BF16)
        number = lane[0:1] + (s * LANES + 1)
        high = (number - (number & 7)).astype(F32)
        low = (number & 7).astype(F32)
        match = row16 == wide(head_tile[s : s + 1], 2 * SUBS)
        parts.append(jnp.concatenate(
            [jnp.where(match, wide(high, 16), 0.0), jnp.where(match, wide(low, 16), 0.0)], axis=0
        ).astype(BF16))
    owner_of = dot_nt(jnp.concatenate(parts, axis=1), hot_head[...])
    owner_of = owner_of[:16] + owner_of[16:]
    free = jnp.where(owner_of == 0.0, 1.0, 0.0).astype(BF16)
    before = dot_nn(free, jnp.where(deep < across, 1.0, 0.0).astype(BF16))
    totals = dot_nn(free, jnp.ones((LANES, LANES), BF16))
    for q in range(atom_rows - 1):
        before = before + jnp.where(row16 > q, wide(totals[q : q + 1], 16), 0.0)
    place_of = jnp.where(owner_of > 0.0, owner_of - 1.0, before + float(bonds)).astype(I32)
    spot = gather(place_of, tail_tile, tail_lane, 0, atom_rows)
    spot = jnp.where(is_far, -1, spot)
    spot_tile, spot_lane = lax.shift_right_arithmetic(spot, 7), spot & (LANES - 1)

    label = jnp.where(is_far, slot, -1)
    for _ in range(ORDER + 1):
        label = jnp.where(is_far, slot, gather(label, spot_tile, spot_lane, -1))
    label_tile, label_lane = lax.shift_right_arithmetic(label, 7), label & (LANES - 1)

    def columns(index, dest):
        col = index.astype(F32).T
        line = lane[0:1].astype(F32)
        for s in range(bond_rows):
            dest[s * LANES : (s + 1) * LANES, :] = jnp.where(
                col[:, s : s + 1] == line, 1.0, 0.0
            ).astype(BF16)

    columns(spot_lane, hot_tail)
    columns(label_lane, hot_root)
    for s in range(bond_rows):
        mask_tail[16 * s : 16 * s + 16, :] = jnp.where(
            row16 == wide(spot_tile[s : s + 1], 16), 1.0, 0.0
        ).astype(BF16)
        for q in range(tiles):
            base = 16 * (s * tiles + q)
            mask_root[base : base + 16, :] = jnp.where(
                wide(label_tile[s : s + 1], 16) == q, 1.0, 0.0
            ).astype(BF16)

    old_pos = old + pos0 + [mass]
    at_head = [gather(v, head_tile, head_lane) for v in old_pos]
    at_tail = [gather(v, tail_tile, tail_lane) for v in old_pos]

    def scatter(rows):
        halves = [half for row in rows for half in split(row)]
        parts = []
        for s in range(bond_rows):
            mask = mask_tail[16 * s : 16 * s + 16, :]
            parts.append(jnp.concatenate(
                [wide(half[s : s + 1], 16).astype(BF16) * mask for half in halves], axis=0
            ))
        out = dot_nn(jnp.concatenate(parts, axis=1), hot_tail[...])
        return [out[32 * i : 32 * i + 16] + out[32 * i + 16 : 32 * i + 32] for i in range(len(rows))]

    def spread(bent, rows):
        pulls = [bent[d] * row for row in rows for d in range(3)]
        sums = scatter(pulls)
        return [
            jnp.concatenate([p - t[:bond_rows], -t[bond_rows:slot_rows]], axis=0)
            for p, t in zip(pulls, sums)
        ], sums

    def meet(moves):
        return [
            mass_head * m[:bond_rows] - near_mass * gather(m, spot_tile, spot_lane) for m in moves
        ]

    def bend(bent, vector):
        return bent[0] * vector[0] + bent[1] * vector[1] + bent[2] * vector[2]

    def to_slots(rows, pieces=2):
        count = -(-len(rows) // SUBS)
        half = SUBS * count
        pad = pieces * count % 2
        for v in range(half):
            stage[SUBS * v : SUBS * v + SUBS, :] = (
                rows[v] if v < len(rows) else jnp.zeros((SUBS, LANES), F32)
            )
        parts = []
        for s in range(bond_rows):
            value = jnp.concatenate(
                [stage[pl.ds(SUBS * SUBS * c + s, SUBS, stride=SUBS), :] for c in range(count)], axis=0
            )
            layers = split(value, pieces) + [jnp.zeros((SUBS, LANES), F32)] * pad
            both = jnp.concatenate(layers, axis=0).astype(BF16)
            size = both.shape[0]
            chunks = []
            for q in range(tiles):
                base = 16 * (s * tiles + q)
                mask = mask_root[base : base + 16, :]
                chunks.append(both * jnp.concatenate([mask] * (size // 16), axis=0))
            parts.append(jnp.concatenate(chunks, axis=0))
        out = dot_nn(jnp.concatenate(parts, axis=1), hot_root[...])
        result = []
        for q in range(tiles):
            found = []
            for c in range(count):
                base = size * q + SUBS * c
                found.append(sum(
                    [out[base + half * p : base + half * p + SUBS] for p in range(1, pieces)],
                    out[base : base + SUBS],
                ))
            result.append(found)
        return result

    def to_bonds(slots, row):
        total = jnp.zeros((bond_rows, LANES), F32)
        for q in range(tiles):
            total = jnp.where(
                label_tile == q, lanes_at(wide(slots[q][row : row + 1], bond_rows), label_lane), total
            )
        return total

    flags = jnp.where(is_far, 1.0, 0.0)
    order = sorted(range(len(classes)), key=lambda r: -(classes[r][0] + classes[r][2]))

    def copies(step, source, landing, offsets, each, whole, merge=True, only=None):
        rows = 0
        for row in only or order:
            if row == centre and not whole or merge and twin and classes[row][1] == 2:
                continue
            line = row if each else 0
            if nowhere(offsets[row]):
                landing[:, row : row + 1, :] = source[:, line : line + 1, :]
                continue
            copy = pltpu.make_async_remote_copy(
                source.at[:, line], landing.at[:, row],
                send_sem.at[step], recv_sem.at[step],
                device_id=target(offsets[row]), device_id_type=MESH,
            )
            copy.start()
            rows += source.shape[0]
        return step, rows

    def post(out, part, value):
        pieces = [value[SUBS * q : SUBS * q + SUBS] for q in range(tiles)]
        if twin:
            pieces[0] = pieces[0] + pieces[1]
            pieces[3] = pieces[3] + jnp.where(sub == 0, wide(pieces[3][1:2]), 0.0)
        for q in range(tiles):
            if not (twin and q == 1):
                out[part, SUBS * q : SUBS * q + SUBS, :] = pieces[q]

    def landed(land, part):
        parts = [land[part, SUBS * q : SUBS * q + SUBS, :] for q in range(tiles)]
        if twin:
            parts[1] = parts[0]
            parts[3] = jnp.where(sub == 1, wide(parts[3][0:1]), parts[3])
        return parts

    pending = []

    def drain(sem, rows):
        lines = spare.at[pl.ds(0, rows)]
        pltpu.make_async_copy(lines, lines, sem).wait()

    def arrive(started):
        step, rows = started
        if rows:
            drain(recv_sem.at[step], rows)
            pending.append(started)


    mass_head = at_head[6]

    def geometry(head_data, tail_data):
        olds = [head_data[d] - tail_data[d] for d in range(3)]
        news = [head_data[3 + d] - tail_data[3 + d] for d in range(3)]
        size = jnp.maximum(jnp.sqrt(olds[0] * olds[0] + olds[1] * olds[1] + olds[2] * olds[2]), 0.5)
        direction = [b / size for b in olds]
        scale = 1.0 / jnp.sqrt(head_data[6] + tail_data[6])
        right = scale * (
            direction[0] * news[0] + direction[1] * news[1] + direction[2] * news[2] - size
        )
        return news, size, scale, [scale * d for d in direction], right

    _, _, _, bent, right = geometry(at_head, at_tail)
    bent = [jnp.where(is_far, 0.0, b) for b in bent]
    near_mass = jnp.where(is_far, 0.0, at_tail[6])
    kids = gather(flags, spot_tile, spot_lane) * near_mass
    series = [jnp.where(is_far, 0.0, right)] + [kids * b for b in bent]
    couplings = [series]
    for k in range(ORDER - 2):
        moves, _ = spread(bent, series)
        meets = meet(moves)
        series = [v - bend(bent, meets[3 * i : 3 * i + 3]) for i, v in enumerate(series)]
        couplings.append(series)
        series = series[:1]
    once = couplings[1][1:]
    zero = couplings[0][1:]
    drive = [[g * couplings[0][0] for g in zero]] + [
        [g * c[0] for g in once] for c in couplings
    ]
    square_of = [
        [left[a] * other[b] for a, b in SYM]
        for left, other in ((zero, zero), (once, zero), (once, once))
    ]

    spread_lane = width * sub + entry

    def to_rows(packed, row):
        return jnp.concatenate(
            [lanes_at(wide(packed[q][row : row + 1]), spread_lane) for q in range(tiles)], axis=0
        )

    drives = to_slots([v for group in drive + square_of for v in group])
    places = to_slots([v * flags for v in at_head], 3)
    for q in range(tiles):
        for c, part in enumerate(places[q] + drives[q]):
            out1[c, SUBS * q : SUBS * q + SUBS, :] = transpose8(part)
    pl.semaphore_wait(barrier, len(greet))
    hub_first = copies(5, out0, in0, direct, False, False, only=(hub_row,))
    second = copies(1, out1, in1, forth, True, False, merge=False)
    others = tuple(row for row in order if row != hub_row)
    first = copies(0, out0, in0, direct, False, False, only=others)

    entry_rows = jnp.concatenate([entry] * tiles, axis=0)
    group_rows = jnp.concatenate([group] * tiles, axis=0)

    def packed(values):
        total = jnp.zeros((SUBS * tiles, LANES), F32)
        for g, value in enumerate(values):
            total = jnp.where(group_rows == g, value, total)
        return total

    def post_terms(values, out):
        steps = [normal[d] * values[k] for k in range(ORDER + 1) for d in range(3)]
        post(out, 0, packed(steps[:SUBS]))
        post(out, 1, packed(steps[SUBS:]))

    arrive(hub_first)
    arrive(second)
    heavy = in0[0, hub_row : hub_row + 1, :] if hub_row != centre else out0[0, 0:1, :]
    sent_data = [lanes_at(wide(heavy), entry + width * g) for g in range(7)]
    mass_send = sent_data[6]
    arrived = [
        lanes_at(in1[v // SUBS], entry_rows + width * (v % SUBS))
        for v in range(SUBS + 3 * ORDER + 6 * (ORDER - 1))
    ]
    head_rows, flat = arrived[:7], arrived[SUBS:]
    drive = [flat[3 * k : 3 * k + 3] for k in range(ORDER)]
    square_of = [flat[3 * ORDER + 6 * k : 3 * ORDER + 6 * k + 6] for k in range(ORDER - 1)]
    _, _, _, normal, start = geometry(
        head_rows, [jnp.concatenate([v] * tiles, axis=0) for v in sent_data]
    )
    normal = [jnp.where(head_rows[6] > 0.0, b, 0.0) for b in normal]
    pairs = [normal[a] * normal[b] for a, b in SYM]
    keep = 1.0 - head_rows[6] * (pairs[0] + pairs[3] + pairs[5])
    pushes = [
        q[0] * pairs[0] + q[3] * pairs[3] + q[5] * pairs[5]
        + 2.0 * (q[1] * pairs[1] + q[2] * pairs[2] + q[4] * pairs[4])
        for q in square_of
    ]
    chain, reply = [start], [None, keep]
    for k in range(1, ORDER + 1):
        value = keep * chain[-1] + (
            normal[0] * drive[k - 1][0] + normal[1] * drive[k - 1][1] + normal[2] * drive[k - 1][2]
        )
        for i in range(k - 1):
            value = value + pushes[k - 2 - i] * chain[i]
        chain.append(value)
    for k in range(2, ORDER):
        value = keep * reply[-1] + pushes[k - 2]
        for i in range(1, k - 1):
            value = value + pushes[k - 2 - i] * reply[i]
        reply.append(value)

    def summed(value):
        total = value[:SUBS]
        for q in range(1, tiles):
            total = total + value[SUBS * q : SUBS * q + SUBS]
        for shift in (4, 2, 1):
            total = total + pltpu.roll(total, shift, 0)
        return total

    got = [summed(normal[d] * chain[k]) for k in range(ORDER + 1) for d in range(3)]
    matrix = [
        {
            ab: -mass_send * summed(p if reply[g] is None else reply[g] * p)
            for ab, p in zip(SYM, pairs)
        }
        for g in range(ORDER)
    ]
    def collect(land):
        found = []
        for part in range(land.shape[0]):
            total = land[part, 0:SUBS, :]
            for q in range(1, tiles):
                if not (twin and q == 1):
                    total = total + land[part, SUBS * q : SUBS * q + SUBS, :]
            for shift in (4, 2, 1):
                total = total + pltpu.roll(total, shift, 0)
            for g in range(SUBS):
                found.append(lanes_at(total, entry + width * g))
        return found

    def owner(got, out):
        moved = []
        for k in range(ORDER + 1):
            total = [-mass_send * got[3 * k + d] for d in range(3)]
            for i in range(k):
                push = matrix[k - 1 - i]
                for d in range(3):
                    for e in range(3):
                        total[d] = total[d] + push[(min(d, e), max(d, e))] * moved[i][e]
            moved.append(total)
        for c in range(2):
            message = jnp.zeros((SUBS, LANES), F32)
            for g in range(SUBS):
                v = SUBS * c + g
                if v < 3 * ORDER:
                    value = moved[v % ORDER][v // ORDER]
                elif v < 3 * ORDER + 3:
                    value = sum([m[v - 3 * ORDER] for m in moved[1:]], moved[0][v - 3 * ORDER])
                else:
                    continue
                message = jnp.where(group == g, value, message)
            out[c] = message

    owner(got, out2)
    third = copies(2, out2, in2, back, False, True)

    arrive(first)
    far = [transpose8(piece) for piece in landed(in0, 0)]
    at_tail = [jnp.where(is_far, to_bonds(far, g), v) for g, v in enumerate(at_tail)]
    bond_new, length, scale, bent, right1 = geometry(at_head, at_tail)
    normal = [part[0] for part in to_slots([b * flags for b in bent])]
    upper = jnp.where(sub < 4, 0, 1)
    normal_a = [subs_at(n, upper) for n in normal]
    normal_b = [wide(n[2:3]) for n in normal]
    normal = [to_rows(normal, d) for d in range(3)]

    terms, fars = [right1], [flags]
    term_moves, term_meets, far_moves, far_meets = [], [], [], []

    def advance():
        moves, _ = spread(bent, [terms[-1], fars[-1]])
        meets = meet(moves)
        term_moves.append(moves[:3])
        far_moves.append(moves[3:])
        term_meets.append(meets[:3])
        far_meets.append(meets[3:])
        terms.append(terms[-1] - bend(bent, meets[:3]))
        fars.append(fars[-1] - bend(bent, meets[3:]))

    for _ in range(ORDER):
        advance()
    last_moves, _ = spread(bent, [terms[ORDER]])
    last_meets = meet(last_moves)
    base1 = sum(terms[1:], terms[0])

    weights, weight_moves, weight_meets = [], [], []
    for k in range(ORDER):
        if k == 0:
            weights.append(fars[0])
            weight_moves.append(far_moves[0])
            weight_meets.append(far_meets[0])
        else:
            weights.append(weights[-1] + fars[k])
            weight_moves.append([a + b for a, b in zip(weight_moves[-1], far_moves[k])])
            weight_meets.append([a + b for a, b in zip(weight_meets[-1], far_meets[k])])
    base_moves = [sum([m[d] for m in term_moves], last_moves[d]) for d in range(3)]
    base_meets = [sum([m[d] for m in term_meets], last_meets[d]) for d in range(3)]

    def answers(land):
        low = [transpose8(piece) for piece in landed(land, 0)]
        high = [transpose8(piece) for piece in landed(land, 1)]
        replies = []
        for q in range(tiles):
            product = low[q] * normal_a[q]
            replies.append(product + pltpu.roll(product, 4, 0) + high[q] * normal_b[q])
        return replies, high

    def through(weights, injected):
        total = weights[0] * injected[ORDER - 1]
        for k in range(1, ORDER):
            total = total + weights[k] * injected[ORDER - 1 - k]
        return total

    arrive(third)
    replies1, high = answers(in2)
    injected1 = [to_bonds(replies1, k) for k in range(ORDER)]
    tail_moves = [to_bonds(high, 4 + d) for d in range(3)]
    sol1 = base1 + through(weights, injected1)
    stretch = [
        bond_new[d]
        - (base_meets[d] + through([w[d] for w in weight_meets], injected1) - flags * tail_moves[d])
        for d in range(3)
    ]
    current = stretch[0] * stretch[0] + stretch[1] * stretch[1] + stretch[2] * stretch[2]
    square = length * length
    goal = jnp.sqrt(jnp.maximum(2.0 * square - current, 0.5 * square))
    right2 = scale * (length - goal)
    slots3 = to_slots([fars[k] * right2 for k in range(ORDER + 1)])
    slots3 = [part[0] for part in slots3]
    post_terms([to_rows(slots3, k) for k in range(ORDER + 1)], out3)
    fourth = copies(3, out3, in3, forth, True, False)

    term, both = right2, sol1 + right2
    for k in range(ORDER + 1):
        moves, _ = spread(bent, [term])
        base_moves = [a + b for a, b in zip(base_moves, moves)]
        if k < ORDER:
            term = term - bend(bent, meet(moves))
            both = both + term
        if k == 1:
            arrive(fourth)
            owner(collect(in3), out4)
            fifth = copies(4, out4, in4, back, False, True)

    place_tile = lax.shift_right_logical(place_of[:atom_rows], 7)
    place_lane = place_of[:atom_rows] & (LANES - 1)
    number = lax.broadcasted_iota(I32, (atom_rows, LANES), 0) * LANES + lax.broadcasted_iota(
        I32, (atom_rows, LANES), 1
    )
    entry_of = jnp.full((atom_rows, LANES), -1, I32)
    for e in range(send_count):
        entry_of = jnp.where(number == wide(send_rep[0:1, e : e + 1] + jnp.zeros((1, LANES), I32), atom_rows), e, entry_of)
    sent = entry_of >= 0
    entry_of = jnp.maximum(entry_of, 0)

    atom_label = jnp.where(
        place_tile < bond_rows, gather(label, place_tile, place_lane, -1, bond_rows), -1
    )
    atom_tile, atom_lane = lax.shift_right_arithmetic(atom_label, 7), atom_label & (LANES - 1)
    at_atoms = [pos0[d] - mass * gather(base_moves[d], place_tile, place_lane) for d in range(3)]
    weight_moves = [
        [mass * gather(w[d][:bond_rows], place_tile, place_lane) for d in range(3)]
        for w in weight_moves
    ]
    early = len(pending)
    for step, rows in pending:
        drain(send_sem.at[step], rows)

    arrive(fifth)
    replies2, _ = answers(in4)
    both = both + through(weights, [to_bonds(replies2, k) for k in range(ORDER)])
    mult_ref[0, 0] = both.reshape(1, bonds)
    replies = [a + b for a, b in zip(replies1, replies2)]
    injected = []
    for k in range(ORDER):
        total = jnp.zeros((atom_rows, LANES), F32)
        for q in range(tiles):
            total = jnp.where(
                atom_tile == q, lanes_at(wide(replies[q][k : k + 1], atom_rows), atom_lane), total
            )
        injected.append(total)
    own = wide(in2[1, centre : centre + 1, :] + in4[1, centre : centre + 1, :], atom_rows)
    for d in range(3):
        result = at_atoms[d] - through([w[d] for w in weight_moves], injected)
        result = result - jnp.where(sent, lanes_at(own, entry_of + width * (4 + d)), 0.0)
        pos_ref[d, 0, 0] = result.reshape(1, atoms)
    for step, rows in pending[early:]:
        drain(send_sem.at[step], rows)


def per_device(axes, sizes, old_pos, displacement, inv_mass, bond_head, bond_tail, send_list):
    atoms, bonds, send_count = old_pos.shape[-1], bond_head.shape[-1], send_list.shape[-1]
    rows = 4 * SUBS
    vmem = lambda *shape: pltpu.VMEM(shape + (LANES,), F32)
    half = lambda *shape: pltpu.VMEM(shape, BF16)
    bond_rows = bonds // LANES
    return pl.pallas_call(
        functools.partial(kernel, axes, sizes, send_count),
        out_shape=(
            pltpu.VMEM(old_pos.shape, F32),
            pltpu.VMEM(bond_head.shape, F32),
        ),
        in_specs=[pl.BlockSpec(memory_space=pltpu.HBM)] * 6,
        out_specs=(pl.BlockSpec(memory_space=pltpu.VMEM), pl.BlockSpec(memory_space=pltpu.VMEM)),
        scratch_shapes=[
            pltpu.VMEM(old_pos.shape, F32), pltpu.VMEM(displacement.shape, F32),
            pltpu.VMEM(inv_mass.shape, F32), pltpu.VMEM(bond_head.shape, I32),
            pltpu.VMEM(bond_tail.shape, I32), pltpu.VMEM(send_list.shape, I32),
            pltpu.SemaphoreType.DMA((6,)),
            vmem(atoms // LANES * SUBS),
            half(LANES, bonds), half(bonds, LANES), half(bonds, LANES),
            half(16 * bond_rows, LANES), half(16 * bond_rows * 4, LANES),
            vmem(4 * SUBS * SUBS),
            vmem(1, SUBS), vmem(1, rows),
            vmem(5, rows), vmem(5, rows),
            vmem(2, SUBS), vmem(2, rows),
            vmem(2, rows), vmem(2, rows),
            vmem(2, SUBS), vmem(2, rows),
            vmem(5 * rows),
            pltpu.SemaphoreType.DMA((6,)),
            pltpu.SemaphoreType.DMA((6,)),
        ],
        compiler_params=pltpu.CompilerParams(
            collective_id=0, has_side_effects=True, vmem_limit_bytes=56 * 1024 * 1024
        ),
    )(old_pos, displacement, inv_mass, bond_head, bond_tail, send_list)


def solution(mesh):
    axes = ("gx", "gy", "gz")
    sizes = tuple(mesh.shape[name] for name in axes)
    return jax.shard_map(
        functools.partial(per_device, axes, sizes),
        mesh=mesh,
        in_specs=(
            P(None, "gx", "gy", "gz", None),
            P(None, "gx", "gy", "gz", None),
            P("gx", "gy", "gz", None),
            P("gx", "gy", "gz", None),
            P("gx", "gy", "gz", None),
            P("gx", "gy", "gz", None),
        ),
        out_specs=(P(None, "gx", "gy", "gz", None), P("gx", "gy", "gz", None)),
        check_vma=False,
    )
```

```python
import functools

import jax
import jax.numpy as jnp
from jax import lax
from jax.experimental import pallas as pl
from jax.experimental.pallas import tpu as pltpu
from jax.sharding import PartitionSpec as P

ORDER = 4
LANES = 128
SUBS = 8
F32, BF16, I32 = jnp.float32, jnp.bfloat16, jnp.int32
MESH = pl.DeviceIdType.MESH
SYM = ((0, 0), (0, 1), (0, 2), (1, 1), (1, 2), (2, 2))


def dot_nt(left, right):
    return lax.dot_general(left, right, (((1,), (1,)), ((), ())), preferred_element_type=F32)


def dot_nn(left, right):
    return lax.dot_general(left, right, (((1,), (0,)), ((), ())), preferred_element_type=F32)


def wide(row, count=SUBS):
    return jnp.broadcast_to(row, (count, row.shape[1]))


def lanes_at(rows, index):
    return jnp.take_along_axis(rows, index, axis=1, mode="promise_in_bounds")


def subs_at(rows, index):
    return jnp.take_along_axis(rows, index, axis=0, mode="promise_in_bounds")


def split(value, count=2):
    parts = []
    for _ in range(count - 1):
        high = value.astype(BF16).astype(F32)
        parts.append(high)
        value = value - high
    return parts + [value]


def flips(n):
    return n >= 4 and n % 2 == 0


def routes(sizes):
    plane = [(a, c) for a in range(3) for c in range(3)]
    classes = [(a, b, c) for b in (0, 2, 1) for a, c in plane[:SUBS]]
    classes += [plane[SUBS][:1] + (b,) + plane[SUBS][1:] for b in (0, 2, 1)]
    forth, back = [], []
    for cls in classes:
        forth.append(tuple((0, 1, -2)[c] if flips(n) else c - 1 for c, n in zip(cls, sizes)))
        back.append(tuple((0, 1, 2)[c] if flips(n) else 1 - c for c, n in zip(cls, sizes)))
    return classes, forth, back


def kernel(
    axes, sizes, send_count,
    old_hbm, move_hbm, mass_hbm, head_hbm, tail_hbm, send_hbm,
    pos_ref, mult_ref,
    old_ref, move_ref, mass_ref, head_ref, tail_ref, send_ref, load_sem,
    table, hot_head, hot_tail, hot_tree, hot_root, mask_tail, mask_tree, mask_root, stage,
    out0, held, in0, out1, in1, out2, in2, out3, in3, out4, in4,
    spare, send_sem, recv_sem,
):
    atoms, bonds = old_ref.shape[-1], head_ref.shape[-1]
    atom_rows, bond_rows = atoms // LANES, bonds // LANES
    slot_rows = bond_rows + -(-(atoms - bonds) // LANES)
    width = send_count
    bits = width.bit_length() - 1
    classes, forth, back = routes(sizes)
    centre = classes.index((1, 1, 1))
    tiles = -(-len(classes) // SUBS)
    here = [lax.axis_index(name) for name in axes]
    turn = [1 - 2 * lax.rem(i, 2) if flips(n) else 1 for i, n in zip(here, sizes)]

    twin = sizes[1] == 2

    def nowhere(offset):
        return all(o % n == 0 for o, n in zip(offset, sizes))

    def target(offset):
        return tuple(
            lax.rem(i + o * s + 2 * n, n) for i, o, s, n in zip(here, offset, turn, sizes)
        )

    greet = []
    for group in (forth, back):
        for offset in group:
            key = tuple(o % n for o, n in zip(offset, sizes))
            if any(key) and key not in [k for k, _ in greet]:
                greet.append((key, offset))
    loads = [
        pltpu.make_async_copy(source, dest, load_sem.at[i])
        for i, (source, dest) in enumerate((
            (send_hbm, send_ref), (old_hbm, old_ref), (move_hbm, move_ref), (mass_hbm, mass_ref),
            (head_hbm, head_ref), (tail_hbm, tail_ref),
        ))
    ]
    for load in loads:
        load.start()
    barrier = pltpu.get_barrier_semaphore()
    for _, offset in greet:
        pl.semaphore_signal(barrier, inc=1, device_id=target(offset), device_id_type=MESH)

    sub = lax.broadcasted_iota(I32, (SUBS, LANES), 0)
    lane = lax.broadcasted_iota(I32, (SUBS, LANES), 1)
    group = lax.shift_right_logical(lane, bits)
    entry = lane & (width - 1)
    swap = (group - sub) & (SUBS - 1)
    unskew = (lane + width * sub) & (LANES - 1)

    def transpose8(x):
        x = pltpu.roll(x, 0, 1, stride=width, stride_axis=0)
        return lanes_at(subs_at(x, swap), unskew)

    for load in loads:
        load.wait()

    old = [old_ref[k, 0, 0].reshape(atom_rows, LANES) for k in range(3)]
    pos0 = [old[k] + move_ref[k, 0, 0].reshape(atom_rows, LANES) for k in range(3)]
    mass = mass_ref[0, 0].reshape(atom_rows, LANES)
    head = head_ref[0, 0].reshape(bond_rows, LANES)
    tail = tail_ref[0, 0].reshape(bond_rows, LANES)
    head_tile, head_lane = lax.shift_right_logical(head, 7), head & (LANES - 1)
    tail_tile, tail_lane = lax.shift_right_logical(tail, 7), tail & (LANES - 1)
    is_far = tail >= atoms
    slot = jnp.maximum(tail - atoms, 0)
    block = lax.shift_right_logical(slot, bits)
    one = lambda test: jnp.where(test, 1, 0)
    bx = one(block >= 9) + one(block >= 18)
    rest = block - 9 * bx
    by = one(rest >= 3) + one(rest >= 6)
    bz = rest - 3 * by
    place = [
        1 - s * (b - 1) if flips(n) else b
        for b, s, n in zip((bx, by, bz), turn, sizes)
    ]
    across_plane = place[0] * 3 + place[2]
    level = jnp.where(place[1] == 0, 0, 3 - place[1])
    slot_row = jnp.where(across_plane < SUBS, SUBS * level + across_plane, 3 * SUBS + level)
    slot = slot_row * width + (slot & (width - 1))

    def gather(rows, tile, index, start=0.0, count=None):
        shape = index.shape
        total = jnp.full(shape, start, rows.dtype)
        for q in range(count or rows.shape[0]):
            total = jnp.where(tile == q, lanes_at(wide(rows[q : q + 1], shape[0]), index), total)
        return total

    deep = lax.broadcasted_iota(I32, (LANES, LANES), 0)
    across = lax.broadcasted_iota(I32, (LANES, LANES), 1)
    row16 = lax.broadcasted_iota(I32, (2 * SUBS, LANES), 0)
    parts = []
    for s in range(bond_rows):
        hot_head[:, s * LANES : (s + 1) * LANES] = jnp.where(
            deep == wide(head_lane[s : s + 1], LANES), 1.0, 0.0
        ).astype(BF16)
        number = lane[0:1] + (s * LANES + 1)
        high = (number - (number & 7)).astype(F32)
        low = (number & 7).astype(F32)
        match = row16 == wide(head_tile[s : s + 1], 2 * SUBS)
        parts.append(jnp.concatenate(
            [jnp.where(match, wide(high, 16), 0.0), jnp.where(match, wide(low, 16), 0.0)], axis=0
        ).astype(BF16))
    owner_of = dot_nt(jnp.concatenate(parts, axis=1), hot_head[...])
    owner_of = owner_of[:16] + owner_of[16:]
    tree = gather(owner_of, tail_tile, tail_lane, 0.0, atom_rows).astype(I32) - 1
    tree = jnp.where(is_far, -1, tree)
    tree_tile, tree_lane = lax.shift_right_arithmetic(tree, 7), tree & (LANES - 1)

    label = jnp.where(is_far, slot, -1)
    for _ in range(ORDER + 1):
        label = jnp.where(is_far, slot, gather(label, tree_tile, tree_lane, -1))
    label_tile, label_lane = lax.shift_right_arithmetic(label, 7), label & (LANES - 1)

    def columns(index, dest):
        col = index.astype(F32).T
        line = lane[0:1].astype(F32)
        for s in range(bond_rows):
            dest[s * LANES : (s + 1) * LANES, :] = jnp.where(
                col[:, s : s + 1] == line, 1.0, 0.0
            ).astype(BF16)

    columns(tree_lane, hot_tree)
    columns(label_lane, hot_root)
    for s in range(bond_rows):
        mask_tree[16 * s : 16 * s + 16, :] = jnp.where(
            (row16 & (SUBS - 1)) == wide(tree_tile[s : s + 1], 16), 1.0, 0.0
        ).astype(BF16)
        for q in range(tiles):
            base = 16 * (s * tiles + q)
            mask_root[base : base + 16, :] = jnp.where(
                wide(label_tile[s : s + 1], 16) == q, 1.0, 0.0
            ).astype(BF16)

    old_pos = old + pos0 + [mass]
    at_head = [gather(v, head_tile, head_lane) for v in old_pos]
    at_tail = [gather(v, tail_tile, tail_lane) for v in old_pos]

    def scatter(rows):
        halves = [half for row in rows for half in split(row)]
        parts = []
        for s in range(bond_rows):
            mask = mask_tail[16 * s : 16 * s + 16, :]
            parts.append(jnp.concatenate(
                [wide(half[s : s + 1], 16).astype(BF16) * mask for half in halves], axis=0
            ))
        out = dot_nn(jnp.concatenate(parts, axis=1), hot_tail[...])
        return [out[32 * i : 32 * i + 16] + out[32 * i + 16 : 32 * i + 32] for i in range(len(rows))]

    def spread(bent, rows):
        pulls = [bent[d] * row for row in rows for d in range(3)]
        sums = scatter(pulls)
        return [
            jnp.concatenate([p - t[:bond_rows], -t[bond_rows:slot_rows]], axis=0)
            for p, t in zip(pulls, sums)
        ]

    def spread_tree(bent, rows):
        pulls = [bent[d] * row for row in rows for d in range(3)]
        halves = [split(pull) for pull in pulls]
        parts = []
        for s in range(bond_rows):
            mask = mask_tree[16 * s : 16 * s + 16, :]
            parts.append(jnp.concatenate([
                jnp.concatenate([wide(half[s : s + 1]) for half in pair], axis=0).astype(BF16) * mask
                for pair in halves
            ], axis=0))
        out = dot_nn(jnp.concatenate(parts, axis=1), hot_tree[...])
        return [
            pull - (out[16 * i : 16 * i + 8] + out[16 * i + 8 : 16 * i + 16])
            for i, pull in enumerate(pulls)
        ]

    def meet_tree(moves):
        return [mass_head * m - near_mass * gather(m, tree_tile, tree_lane) for m in moves]

    def meet(moves):
        return [
            mass_head * m[:bond_rows] - near_mass * gather(m, spot_tile, spot_lane) for m in moves
        ]

    def bend(bent, vector):
        return bent[0] * vector[0] + bent[1] * vector[1] + bent[2] * vector[2]

    def to_slots(rows, pieces=2):
        count = -(-len(rows) // SUBS)
        half = SUBS * count
        pad = pieces * count % 2
        for v in range(half):
            stage[SUBS * v : SUBS * v + SUBS, :] = (
                rows[v] if v < len(rows) else jnp.zeros((SUBS, LANES), F32)
            )
        parts = []
        for s in range(bond_rows):
            value = jnp.concatenate(
                [stage[pl.ds(SUBS * SUBS * c + s, SUBS, stride=SUBS), :] for c in range(count)], axis=0
            )
            layers = split(value, pieces) + [jnp.zeros((SUBS, LANES), F32)] * pad
            both = jnp.concatenate(layers, axis=0).astype(BF16)
            size = both.shape[0]
            chunks = []
            for q in range(tiles):
                base = 16 * (s * tiles + q)
                mask = mask_root[base : base + 16, :]
                chunks.append(both * jnp.concatenate([mask] * (size // 16), axis=0))
            parts.append(jnp.concatenate(chunks, axis=0))
        out = dot_nn(jnp.concatenate(parts, axis=1), hot_root[...])
        result = []
        for q in range(tiles):
            found = []
            for c in range(count):
                base = size * q + SUBS * c
                found.append(sum(
                    [out[base + half * p : base + half * p + SUBS] for p in range(1, pieces)],
                    out[base : base + SUBS],
                ))
            result.append(found)
        return result

    def to_bonds(slots, row):
        total = jnp.zeros((bond_rows, LANES), F32)
        for q in range(tiles):
            total = jnp.where(
                label_tile == q, lanes_at(wide(slots[q][row : row + 1], bond_rows), label_lane), total
            )
        return total

    flags = jnp.where(is_far, 1.0, 0.0)
    order = sorted(
        range(len(classes)),
        key=lambda r: -(4 * min(classes[r][0], 1) + 4 * classes[r][2] + abs(classes[r][1] - 1)),
    )

    def copies(step, source, landing, offsets, each, whole, merge=True):
        rows = 0
        for row in order:
            if row == centre and not whole or merge and twin and classes[row][1] == 2:
                continue
            line = row if each else 0
            if nowhere(offsets[row]):
                landing[:, row : row + 1, :] = source[:, line : line + 1, :]
                continue
            copy = pltpu.make_async_remote_copy(
                source.at[:, line], landing.at[:, row],
                send_sem.at[step], recv_sem.at[step],
                device_id=target(offsets[row]), device_id_type=MESH,
            )
            copy.start()
            rows += source.shape[0]
        return step, rows

    def post(out, part, value):
        pieces = [value[SUBS * q : SUBS * q + SUBS] for q in range(tiles)]
        if twin:
            pieces[0] = pieces[0] + pieces[1]
            pieces[3] = pieces[3] + jnp.where(sub == 0, wide(pieces[3][1:2]), 0.0)
        for q in range(tiles):
            if not (twin and q == 1):
                out[part, SUBS * q : SUBS * q + SUBS, :] = pieces[q]

    def landed(land, part):
        parts = [land[part, SUBS * q : SUBS * q + SUBS, :] for q in range(tiles)]
        if twin:
            parts[1] = parts[0]
            parts[3] = jnp.where(sub == 1, wide(parts[3][0:1]), parts[3])
        return parts

    pending = []

    def drain(sem, rows):
        lines = spare.at[pl.ds(0, rows)]
        pltpu.make_async_copy(lines, lines, sem).wait()

    def arrive(started):
        step, rows = started
        if rows:
            drain(recv_sem.at[step], rows)
            pending.append(started)


    mass_head = at_head[6]

    def geometry(head_data, tail_data):
        olds = [head_data[d] - tail_data[d] for d in range(3)]
        news = [head_data[3 + d] - tail_data[3 + d] for d in range(3)]
        size = jnp.maximum(jnp.sqrt(olds[0] * olds[0] + olds[1] * olds[1] + olds[2] * olds[2]), 0.5)
        direction = [b / size for b in olds]
        scale = 1.0 / jnp.sqrt(head_data[6] + tail_data[6])
        right = scale * (
            direction[0] * news[0] + direction[1] * news[1] + direction[2] * news[2] - size
        )
        return news, size, scale, [scale * d for d in direction], right

    near_new, near_length, near_scale, near, right = geometry(at_head, at_tail)
    near = [jnp.where(is_far, 0.0, b) for b in near]
    near_mass = jnp.where(is_far, 0.0, at_tail[6])
    kids = gather(flags, tree_tile, tree_lane) * near_mass
    series = [jnp.where(is_far, 0.0, right)] + [kids * b for b in near]

    def advance(series, spread=spread_tree, meet=meet_tree):
        moves = spread(near, series)
        meets = meet(moves)
        return [
            v - bend(near, meets[3 * i : 3 * i + 3]) for i, v in enumerate(series)
        ], moves, meets

    couplings = [series]
    for k in range(ORDER - 2):
        series, moves, meets = advance(series)
        if k == 0:
            unit_moves, unit_meets = [moves[3:]], [meets[3:]]
        couplings.append(series)
        series = series[:1]
    once = couplings[1][1:]
    zero = couplings[0][1:]
    drive = [[g * couplings[0][0] for g in zero]] + [
        [g * c[0] for g in once] for c in couplings
    ]
    square_of = [
        [left[a] * other[b] for a, b in SYM]
        for left, other in ((zero, zero), (once, zero), (once, once))
    ]

    spread_lane = width * sub + entry

    def to_rows(packed, row):
        return jnp.concatenate(
            [lanes_at(wide(packed[q][row : row + 1]), spread_lane) for q in range(tiles)], axis=0
        )

    drives = to_slots([v for group in drive + square_of for v in group])
    places = to_slots([v * flags for v in at_head], 3)
    for q in range(tiles):
        for c, part in enumerate(places[q] + drives[q]):
            out1[c, SUBS * q : SUBS * q + SUBS, :] = transpose8(part)
    pl.semaphore_wait(barrier, len(greet))
    second = copies(1, out1, in1, forth, True, False, merge=False)

    values = old + pos0 + [mass, jnp.zeros((atom_rows, LANES), F32)]
    for g, value in enumerate(values):
        for q in range(atom_rows):
            table[SUBS * q + g : SUBS * q + g + 1, :] = value[q : q + 1]
    send_row = jnp.concatenate(
        [send_ref[0, 0], jnp.zeros((1, LANES - send_count), I32)], axis=1
    )
    send_rep = lanes_at(wide(send_row), entry)
    send_tile, send_lane = lax.shift_right_logical(send_rep, 7), send_rep & (LANES - 1)
    found = jnp.zeros((SUBS, LANES), F32)
    for q in range(atom_rows):
        found = jnp.where(
            send_tile == q, lanes_at(table[SUBS * q : SUBS * q + SUBS, :], send_lane), found
        )
    found = jnp.sum(jnp.where(group == sub, found, 0.0), axis=0, keepdims=True)
    out0[0] = wide(found)
    for land in (in1, in3):
        for part in range(land.shape[0]):
            land[part, centre : centre + 1, :] = jnp.zeros((1, LANES), F32)
            land[part, len(classes) :, :] = jnp.zeros((SUBS * tiles - len(classes), LANES), F32)
            if twin and land is in3:
                land[part, 3 * SUBS + 1 : 3 * SUBS + 2, :] = jnp.zeros((1, LANES), F32)
    if nowhere(forth[centre]):
        to_hub = 5, 0
        held[...] = out0[...]
    else:
        pltpu.make_async_remote_copy(
            out0.at[:, 0], held.at[:, 0], send_sem.at[5], recv_sem.at[5],
            device_id=target(forth[centre]), device_id_type=MESH,
        ).start()
        to_hub = 5, 1

    free = jnp.where(owner_of == 0.0, 1.0, 0.0).astype(BF16)
    before = dot_nn(free, jnp.where(deep < across, 1.0, 0.0).astype(BF16))
    totals = dot_nn(free, jnp.ones((LANES, LANES), BF16))
    for q in range(atom_rows - 1):
        before = before + jnp.where(row16 > q, wide(totals[q : q + 1], 16), 0.0)
    place_of = jnp.where(owner_of > 0.0, owner_of - 1.0, before + float(bonds)).astype(I32)
    spot = gather(place_of, tail_tile, tail_lane, 0, atom_rows)
    spot = jnp.where(is_far, -1, spot)
    spot_tile, spot_lane = lax.shift_right_arithmetic(spot, 7), spot & (LANES - 1)
    columns(spot_lane, hot_tail)
    for s in range(bond_rows):
        mask_tail[16 * s : 16 * s + 16, :] = jnp.where(
            row16 == wide(spot_tile[s : s + 1], 16), 1.0, 0.0
        ).astype(BF16)

    def powers(normal, mass_at, start, drive, square_of, last):
        pairs = [normal[a] * normal[b] for a, b in SYM]
        keep = 1.0 - mass_at * (pairs[0] + pairs[3] + pairs[5])
        pushes = [
            q[0] * pairs[0] + q[3] * pairs[3] + q[5] * pairs[5]
            + 2.0 * (q[1] * pairs[1] + q[2] * pairs[2] + q[4] * pairs[4])
            for q in square_of
        ]
        chain, reply = [start], [None, keep]
        for k in range(1, ORDER + 1):
            value = keep * chain[-1] + bend(normal, drive[k - 1])
            for i in range(k - 1):
                value = value + pushes[k - 2 - i] * chain[i]
            chain.append(value)
        for k in range(2, last + 1):
            value = keep * reply[-1] + pushes[k - 2]
            for i in range(1, k - 1):
                value = value + pushes[k - 2 - i] * reply[i]
            reply.append(value)
        return pairs, chain, reply

    units = [zero, once]
    rights = [couplings[0][0]]
    for k in range(ORDER):
        series, _, _ = advance(rights[-1:], spread, meet)
        rights += series
        if k:
            series, moves, meets = advance(units[k])
            unit_moves.append(moves)
            unit_meets.append(meets)
            units.append(series)
    near_sum = sum(rights[1:], rights[0])
    near_moves = spread(near, [near_sum])
    near_meets = meet(near_moves)
    root_head = [to_bonds([part[0] for part in places], g) for g in range(7)]
    root_flat = [
        to_bonds([part[v // SUBS] for part in drives], v % SUBS)
        for v in range(3 * ORDER + 6 * (ORDER - 1))
    ]

    entry_rows = jnp.concatenate([entry] * tiles, axis=0)
    group_rows = jnp.concatenate([group] * tiles, axis=0)

    def packed(values):
        total = jnp.zeros((SUBS * tiles, LANES), F32)
        for g, value in enumerate(values):
            total = jnp.where(group_rows == g, value, total)
        return total

    def post_terms(values, out):
        steps = [normal[d] * values[k] for k in range(ORDER + 1) for d in range(3)]
        post(out, 0, packed(steps[:SUBS]))
        post(out, 1, packed(steps[SUBS:]))

    arrive(to_hub)
    first = copies(0, held, in0, back, False, False)
    arrive(second)
    sent_data = [lanes_at(wide(held[0, 0:1, :]), entry + width * g) for g in range(7)]
    mass_send = sent_data[6]
    arrived = [
        lanes_at(in1[v // SUBS], entry_rows + width * (v % SUBS))
        for v in range(SUBS + 3 * ORDER + 6 * (ORDER - 1))
    ]
    head_rows, flat = arrived[:7], arrived[SUBS:]
    drive = [flat[3 * k : 3 * k + 3] for k in range(ORDER)]
    square_of = [flat[3 * ORDER + 6 * k : 3 * ORDER + 6 * k + 6] for k in range(ORDER - 1)]
    _, _, _, normal, start = geometry(
        head_rows, [jnp.concatenate([v] * tiles, axis=0) for v in sent_data]
    )
    normal = [jnp.where(head_rows[6] > 0.0, b, 0.0) for b in normal]
    pairs, chain, reply = powers(normal, head_rows[6], start, drive, square_of, ORDER - 1)

    def summed(value):
        total = value[:SUBS]
        for q in range(1, tiles):
            total = total + value[SUBS * q : SUBS * q + SUBS]
        for shift in (4, 2, 1):
            total = total + pltpu.roll(total, shift, 0)
        return total

    got = [summed(normal[d] * chain[k]) for k in range(ORDER + 1) for d in range(3)]
    matrix = [
        {
            ab: -mass_send * summed(p if reply[g] is None else reply[g] * p)
            for ab, p in zip(SYM, pairs)
        }
        for g in range(ORDER)
    ]
    def collect(land):
        found = []
        for part in range(land.shape[0]):
            total = land[part, 0:SUBS, :]
            for q in range(1, tiles):
                if not (twin and q == 1):
                    total = total + land[part, SUBS * q : SUBS * q + SUBS, :]
            for shift in (4, 2, 1):
                total = total + pltpu.roll(total, shift, 0)
            for g in range(SUBS):
                found.append(lanes_at(total, entry + width * g))
        return found

    def owner(got, out):
        moved = []
        for k in range(ORDER + 1):
            total = [-mass_send * got[3 * k + d] for d in range(3)]
            for i in range(k):
                push = matrix[k - 1 - i]
                for d in range(3):
                    for e in range(3):
                        total[d] = total[d] + push[(min(d, e), max(d, e))] * moved[i][e]
            moved.append(total)
        for c in range(2):
            message = jnp.zeros((SUBS, LANES), F32)
            for g in range(SUBS):
                v = SUBS * c + g
                if v < 3 * ORDER:
                    value = moved[v % ORDER][v // ORDER]
                elif v < 3 * ORDER + 3:
                    value = sum([m[v - 3 * ORDER] for m in moved[1:]], moved[0][v - 3 * ORDER])
                else:
                    continue
                message = jnp.where(group == g, value, message)
            out[c] = message

    owner(got, out2)
    third = copies(2, out2, in2, back, False, True)

    arrive(first)
    far = [transpose8(piece) for piece in landed(in0, 0)]
    root_new, root_length, root_scale, root, start = geometry(
        root_head, [to_bonds(far, g) for g in range(7)]
    )
    rooted = label >= 0
    root = [jnp.where(rooted, b, 0.0) for b in root]
    normal = [part[0] for part in to_slots([b * flags for b in root])]
    upper = jnp.where(sub < 4, 0, 1)
    normal_a = [subs_at(n, upper) for n in normal]
    normal_b = [wide(n[2:3]) for n in normal]
    normal = [to_rows(normal, d) for d in range(3)]

    _, chain, reply = powers(
        root, root_head[6], jnp.where(rooted, start, 0.0),
        [root_flat[3 * k : 3 * k + 3] for k in range(ORDER)],
        [root_flat[3 * ORDER + 6 * k : 3 * ORDER + 6 * k + 6] for k in range(ORDER - 1)], ORDER,
    )
    reply[0] = jnp.ones((bond_rows, LANES), F32)
    bond_new = [jnp.where(is_far, a, b) for a, b in zip(root_new, near_new)]
    length = jnp.where(is_far, root_length, near_length)
    scale = jnp.where(is_far, root_scale, near_scale)
    bent = [jnp.where(is_far, a, b) for a, b in zip(root, near)]
    own_meet = flags * mass_head - kids

    def rooted_sum(part):
        return [
            sum([root[e] * part[3 * e + d][:bond_rows] for e in (1, 2)], root[0] * part[d][:bond_rows])
            for d in range(3)
        ]

    unit_sums = [bend(root, unit) for unit in units[:ORDER]]
    unit_moves = [rooted_sum(part) for part in unit_moves]
    unit_meets = [rooted_sum(part) for part in unit_meets]

    def combine(first, factors, parts):
        for factor, part in zip(factors, parts):
            first = first + factor * part
        return first

    fars, far_moves, far_meets = [], [], []
    for k in range(ORDER + 1):
        back_k = reply[:k][::-1]
        fars.append(combine(flags * reply[k], back_k, unit_sums))
        far_moves.append([
            combine(flags * reply[k] * root[d], back_k, [m[d] for m in unit_moves]) for d in range(3)
        ])
        far_meets.append([
            combine(own_meet * reply[k] * root[d], back_k, [m[d] for m in unit_meets])
            for d in range(3)
        ])
    totals = [chain[0]]
    for k in range(1, ORDER + 1):
        totals.append(totals[-1] + chain[k])
    back_k = totals[:ORDER][::-1]
    base1 = near_sum + combine(flags * totals[ORDER], back_k, unit_sums)
    base_moves = [
        jnp.concatenate([
            near_moves[d][:bond_rows]
            + combine(flags * totals[ORDER] * root[d], back_k, [m[d] for m in unit_moves]),
            near_moves[d][bond_rows:],
        ], axis=0)
        for d in range(3)
    ]
    base_meets = [
        near_meets[d]
        + combine(own_meet * totals[ORDER] * root[d], back_k, [m[d] for m in unit_meets])
        for d in range(3)
    ]

    weights, weight_moves, weight_meets = [], [], []
    for k in range(ORDER):
        if k == 0:
            weights.append(fars[0])
            weight_moves.append(far_moves[0])
            weight_meets.append(far_meets[0])
        else:
            weights.append(weights[-1] + fars[k])
            weight_moves.append([a + b for a, b in zip(weight_moves[-1], far_moves[k])])
            weight_meets.append([a + b for a, b in zip(weight_meets[-1], far_meets[k])])
    def answers(land):
        low = [transpose8(piece) for piece in landed(land, 0)]
        high = [transpose8(piece) for piece in landed(land, 1)]
        replies = []
        for q in range(tiles):
            product = low[q] * normal_a[q]
            replies.append(product + pltpu.roll(product, 4, 0) + high[q] * normal_b[q])
        return replies, high

    def through(weights, injected):
        total = weights[0] * injected[ORDER - 1]
        for k in range(1, ORDER):
            total = total + weights[k] * injected[ORDER - 1 - k]
        return total

    arrive(third)
    replies1, high = answers(in2)
    injected1 = [to_bonds(replies1, k) for k in range(ORDER)]
    tail_moves = [to_bonds(high, 4 + d) for d in range(3)]
    sol1 = base1 + through(weights, injected1)
    stretch = [
        bond_new[d]
        - (base_meets[d] + through([w[d] for w in weight_meets], injected1) - flags * tail_moves[d])
        for d in range(3)
    ]
    current = stretch[0] * stretch[0] + stretch[1] * stretch[1] + stretch[2] * stretch[2]
    square = length * length
    goal = jnp.sqrt(jnp.maximum(2.0 * square - current, 0.5 * square))
    right2 = scale * (length - goal)
    slots3 = to_slots([fars[k] * right2 for k in range(ORDER + 1)])
    slots3 = [part[0] for part in slots3]
    post_terms([to_rows(slots3, k) for k in range(ORDER + 1)], out3)
    fourth = copies(3, out3, in3, forth, True, False)

    term, both = right2, sol1 + right2
    for k in range(ORDER + 1):
        moves = spread(bent, [term])
        base_moves = [a + b for a, b in zip(base_moves, moves)]
        if k < ORDER:
            term = term - bend(bent, meet(moves))
            both = both + term
        if k == 1:
            arrive(fourth)
            owner(collect(in3), out4)
            fifth = copies(4, out4, in4, back, False, True)

    place_tile = lax.shift_right_logical(place_of[:atom_rows], 7)
    place_lane = place_of[:atom_rows] & (LANES - 1)
    number = lax.broadcasted_iota(I32, (atom_rows, LANES), 0) * LANES + lax.broadcasted_iota(
        I32, (atom_rows, LANES), 1
    )
    entry_of = jnp.full((atom_rows, LANES), -1, I32)
    for e in range(send_count):
        entry_of = jnp.where(number == wide(send_rep[0:1, e : e + 1] + jnp.zeros((1, LANES), I32), atom_rows), e, entry_of)
    sent = entry_of >= 0
    entry_of = jnp.maximum(entry_of, 0)

    atom_label = jnp.where(
        place_tile < bond_rows, gather(label, place_tile, place_lane, -1, bond_rows), -1
    )
    atom_tile, atom_lane = lax.shift_right_arithmetic(atom_label, 7), atom_label & (LANES - 1)
    at_atoms = [pos0[d] - mass * gather(base_moves[d], place_tile, place_lane) for d in range(3)]
    weight_moves = [
        [mass * gather(w[d][:bond_rows], place_tile, place_lane) for d in range(3)]
        for w in weight_moves
    ]
    early = len(pending)
    for step, rows in pending:
        drain(send_sem.at[step], rows)

    arrive(fifth)
    replies2, _ = answers(in4)
    both = both + through(weights, [to_bonds(replies2, k) for k in range(ORDER)])
    mult_ref[0, 0] = both.reshape(1, bonds)
    replies = [a + b for a, b in zip(replies1, replies2)]
    injected = []
    for k in range(ORDER):
        total = jnp.zeros((atom_rows, LANES), F32)
        for q in range(tiles):
            total = jnp.where(
                atom_tile == q, lanes_at(wide(replies[q][k : k + 1], atom_rows), atom_lane), total
            )
        injected.append(total)
    own = wide(in2[1, centre : centre + 1, :] + in4[1, centre : centre + 1, :], atom_rows)
    for d in range(3):
        result = at_atoms[d] - through([w[d] for w in weight_moves], injected)
        result = result - jnp.where(sent, lanes_at(own, entry_of + width * (4 + d)), 0.0)
        pos_ref[d, 0, 0] = result.reshape(1, atoms)
    for step, rows in pending[early:]:
        drain(send_sem.at[step], rows)


def per_device(axes, sizes, old_pos, displacement, inv_mass, bond_head, bond_tail, send_list):
    atoms, bonds, send_count = old_pos.shape[-1], bond_head.shape[-1], send_list.shape[-1]
    rows = 4 * SUBS
    vmem = lambda *shape: pltpu.VMEM(shape + (LANES,), F32)
    half = lambda *shape: pltpu.VMEM(shape, BF16)
    bond_rows = bonds // LANES
    return pl.pallas_call(
        functools.partial(kernel, axes, sizes, send_count),
        out_shape=(
            pltpu.VMEM(old_pos.shape, F32),
            pltpu.VMEM(bond_head.shape, F32),
        ),
        in_specs=[pl.BlockSpec(memory_space=pltpu.HBM)] * 6,
        out_specs=(pl.BlockSpec(memory_space=pltpu.VMEM), pl.BlockSpec(memory_space=pltpu.VMEM)),
        scratch_shapes=[
            pltpu.VMEM(old_pos.shape, F32), pltpu.VMEM(displacement.shape, F32),
            pltpu.VMEM(inv_mass.shape, F32), pltpu.VMEM(bond_head.shape, I32),
            pltpu.VMEM(bond_tail.shape, I32), pltpu.VMEM(send_list.shape, I32),
            pltpu.SemaphoreType.DMA((6,)),
            vmem(atoms // LANES * SUBS),
            half(LANES, bonds), half(bonds, LANES), half(bonds, LANES), half(bonds, LANES),
            half(16 * bond_rows, LANES), half(16 * bond_rows, LANES),
            half(16 * bond_rows * 4, LANES),
            vmem(4 * SUBS * SUBS),
            vmem(1, SUBS), vmem(1, SUBS), vmem(1, rows),
            vmem(5, rows), vmem(5, rows),
            vmem(2, SUBS), vmem(2, rows),
            vmem(2, rows), vmem(2, rows),
            vmem(2, SUBS), vmem(2, rows),
            vmem(5 * rows),
            pltpu.SemaphoreType.DMA((6,)),
            pltpu.SemaphoreType.DMA((6,)),
        ],
        compiler_params=pltpu.CompilerParams(
            collective_id=0, has_side_effects=True, vmem_limit_bytes=56 * 1024 * 1024
        ),
    )(old_pos, displacement, inv_mass, bond_head, bond_tail, send_list)


def solution(mesh):
    axes = ("gx", "gy", "gz")
    sizes = tuple(mesh.shape[name] for name in axes)
    return jax.shard_map(
        functools.partial(per_device, axes, sizes),
        mesh=mesh,
        in_specs=(
            P(None, "gx", "gy", "gz", None),
            P(None, "gx", "gy", "gz", None),
            P("gx", "gy", "gz", None),
            P("gx", "gy", "gz", None),
            P("gx", "gy", "gz", None),
            P("gx", "gy", "gz", None),
        ),
        out_specs=(P(None, "gx", "gy", "gz", None), P("gx", "gy", "gz", None)),
        check_vma=False,
    )
```
